32 devices in a mesh: grp: 16 (over z, y, x), loc: 2 (over core).
Axes of the slice: x: 2, y: 2, z: 4, core: 2. Of those that a mesh axis runs over, the one named last changes fastest.
Arguments:
- tokens: bfloat16 [1024, 3584], P(('grp', 'loc')), may hold values from -6 to 6
- gate_weights: bfloat16 [1024, 8], P(('grp', 'loc')), may hold values from 0.099609375 to 0.59765625
- expert_ids: int32 [1024, 8], P(('grp', 'loc')), may hold values from 0 to 31, as said below
- w_gate: bfloat16 [32, 3584, 1024], P('grp', None, 'loc'), may hold values from -0.09375 to 0.09375
- w_up: bfloat16 [32, 3584, 1024], P('grp', None, 'loc'), may hold values from -0.09375 to 0.09375
- w_down: bfloat16 [32, 3584, 1024], P('grp', None, 'loc'), may hold values from -0.1875 to 0.1875
Outputs:
- layer_out: bfloat16 [1024, 3584], P(('grp', 'loc'))
The draws below stay inside these ranges and needn't reach their ends.
Inputs may be any that keep to these rules, and one draw needn't show every extreme that they name: `expert_ids`: each row names 8 different experts: two in each of 4 different routing groups, a routing group being 4 consecutive expert numbers. Among the rows of one device (aligned blocks of 32 rows) each expert is named at most 16 times, and in every such block some expert is named exactly 16 times.
All inputs are finite; a program needn't handle non-finite values.
Results may differ from the reference program's by a relative error of at most 0.01.
Values may be sent and summed in bfloat16 or wider, within the bound.
A program may use at most 192 MiB of HBM per device.

```python
import jax
import jax.numpy as jnp
from jax import lax

D = 3584
FFE = 1024
RGROUPS = 8
TOPG = 4
TOPK = 8
TOK_DEV = 32
EXPERTS = 32
TOKENS = 1024
MOST = 16
N_LOC = 2


def draw_expert_ids(key, part):
    group_span = EXPERTS // RGROUPS
    block_count = TOKENS // TOK_DEV
    key_first = jax.random.fold_in(key, 11)
    key_second = jax.random.fold_in(key, 12)
    key_rank = jax.random.fold_in(key, 13)
    key_rotation = jax.random.fold_in(key, 14)
    hot_first = jax.random.randint(key_first, (block_count,), 0, RGROUPS)
    hot_second = jax.random.randint(key_second, (block_count,), 0, RGROUPS)
    hot_group = jnp.repeat(jnp.minimum(hot_first, hot_second), TOK_DEV)
    group_index = jnp.arange(RGROUPS, dtype=jnp.int32)
    scores = jax.random.randint(key_rank, (TOKENS, RGROUPS), 0, 1 << 20) * RGROUPS + group_index[None, :]
    scores = jnp.where(group_index[None, :] == hot_group[:, None], 1 << 30, scores)
    chosen = lax.top_k(scores, TOPG)[1].astype(jnp.int32)
    member = jnp.sum((chosen[:, :, None] == group_index[None, None, :]).astype(jnp.int32), axis=1)
    member = member.reshape(block_count, TOK_DEV, RGROUPS)
    order_rank = jnp.cumsum(member, axis=1) - member
    rotation = jax.random.randint(key_rotation, (block_count, 1, RGROUPS), 0, group_span)
    first_local = ((rotation + order_rank) % group_span).reshape(TOKENS, RGROUPS)
    first_pick = jnp.take_along_axis(first_local, chosen, axis=1)
    second_pick = (first_pick + group_span // 2) % group_span
    group_base = chosen * group_span
    expert_pick = jnp.stack([group_base + first_pick, group_base + second_pick], axis=2)
    return expert_pick.reshape(TOKENS, TOPK).astype(jnp.int32)


def shard_levels(rng, extent, pieces, least, high):
    def one(position, parts):
        heights = jax.random.uniform(jax.random.fold_in(jax.random.fold_in(rng, 6), position), (parts,), jnp.float32, least / len(pieces), high / len(pieces))
        return jnp.repeat(jnp.exp(heights), extent[position] // parts).reshape((-1,) + (1,) * (len(extent) - position - 1))

    level = one(*pieces[0])
    for cut in pieces[1:]:
        level = level * one(*cut)
    return level


def centred(own_key, extent, scale, limit, shards=(), kind=jnp.bfloat16):
    values = jax.random.normal(own_key, extent, jnp.float32) * scale
    if len(shards) > 0:
        values = shard_levels(own_key, extent, shards, -0.22, 0.18) * values
    return jnp.clip(values, min=-limit, max=limit).astype(kind)


def setup_inputs(seed: int = 0) -> dict:
    streams_of = jax.random.split(jax.random.key(seed), 7)
    tokens = centred(streams_of[0], (TOKENS, D), 1.0, 6.0, ((0, 32),))
    gate_weights = jnp.clip(0.099609375 + 0.49804688 * jax.random.uniform(streams_of[1], (TOKENS, TOPK), jnp.float32) ** shard_levels(streams_of[1], (TOKENS, TOPK), ((0, 32),), -0.2, 0.2), 0.099609375, 0.59765625).astype(jnp.bfloat16)
    expert_ids = draw_expert_ids(jax.random.fold_in(streams_of[6], 71), 0)
    w_gate = centred(streams_of[3], (EXPERTS, D, FFE), D ** -0.5, 0.09375, ((0, 16), (2, 2)))
    w_up = centred(streams_of[4], (EXPERTS, D, FFE), D ** -0.5, 0.09375, ((0, 16), (2, 2)))
    w_down = centred(streams_of[5], (EXPERTS, D, FFE), FFE ** -0.5, 0.1875, ((0, 16), (2, 2)))
    return dict(tokens=tokens, gate_weights=gate_weights, expert_ids=expert_ids, w_gate=w_gate, w_up=w_up, w_down=w_down)


def reference(tokens, gate_weights, expert_ids, w_gate, w_up, w_down):
    block_count = TOKENS // TOK_DEV
    pair_block = TOK_DEV * TOPK
    per_expert = block_count * MOST
    shard_units = FFE // N_LOC
    block_ids = expert_ids.reshape(block_count, pair_block).astype(jnp.int32)
    same_expert = (block_ids[:, :, None] == block_ids[:, None, :]).astype(jnp.int32)
    pair_order = jnp.arange(pair_block, dtype=jnp.int32)
    earlier = (pair_order[:, None] > pair_order[None, :]).astype(jnp.int32)
    slot_rank = jnp.sum(same_expert * earlier[None], axis=2).astype(jnp.int32)
    block_index = jnp.arange(block_count, dtype=jnp.int32)[:, None]
    target = (block_ids * per_expert + block_index * MOST + slot_rank).reshape(-1).astype(jnp.int32)
    pair_index = jnp.arange(TOKENS * TOPK, dtype=jnp.int32)
    slot_table = jnp.full((EXPERTS * per_expert,), -1, jnp.int32).at[target].set(pair_index)
    slot_table = slot_table.reshape(EXPERTS, per_expert)
    flat_scales = gate_weights.reshape(-1)

    def one_expert(totals, inputs):
        index_row, gate_part, up_part, down_part = inputs
        is_valid = index_row >= 0
        safe_index = jnp.maximum(index_row, 0).astype(jnp.int32)
        token_row = (safe_index // TOPK).astype(jnp.int32)
        rows_in = tokens[token_row]
        scales = jnp.where(is_valid, flat_scales[safe_index].astype(jnp.float32), jnp.zeros((), jnp.float32))
        gate_act = jnp.dot(rows_in, gate_part, preferred_element_type=jnp.float32)
        upward = jnp.dot(rows_in, up_part, preferred_element_type=jnp.float32)
        hidden = (jax.nn.silu(gate_act) * upward).astype(jnp.bfloat16)
        blocked = hidden.reshape(per_expert, N_LOC, shard_units).astype(jnp.float32)
        down_blocks = down_part.reshape(D, N_LOC, shard_units).astype(jnp.float32)
        partial_value = jnp.einsum("rlf,dlf->rld", blocked, down_blocks)
        partial_value = lax.optimization_barrier((partial_value * scales[:, None, None]).astype(jnp.bfloat16))
        outcome = jnp.sum(partial_value.astype(jnp.float32), axis=1).astype(jnp.bfloat16)
        outcome = lax.optimization_barrier(outcome)
        return totals.at[token_row].add(outcome.astype(jnp.float32)), None

    start_totals = jnp.zeros((TOKENS, D), jnp.float32)
    totals = lax.scan(one_expert, start_totals, (slot_table, w_gate, w_up, w_down))[0]
    return totals.astype(jnp.bfloat16)
```

```python
import functools

import jax
import jax.numpy as jnp
from jax import lax
from jax.experimental import pallas as pl
from jax.experimental.pallas import tpu as pltpu
from jax.sharding import PartitionSpec as P

RGROUPS = 8
LANES = 128
TILE = 256
MESH = pl.DeviceIdType.MESH
FLIPS = ((1, 0), (0, 1))
HERE, DIAG = (0, 0), (1, 1)


class Place:
    def __init__(self, columns):
        self.deep = columns // 4
        self.g = lax.axis_index("grp")
        self.c = lax.axis_index("loc")
        self.x = lax.rem(self.g, 2)
        self.y = lax.rem(lax.div(self.g, 2), 2)
        self.z = lax.div(self.g, 4)
        self.below = self.z > 0
        self.above = self.z < self.deep - 1

    def spot(self, flip):
        x = 1 - self.x if flip[0] else self.x
        y = 1 - self.y if flip[1] else self.y
        return y * 2 + x

    def at(self, dz=0, flip=HERE):
        return (self.z + dz) * 4 + self.spot(flip)

    def line(self, step):
        if step == 0:
            return [(0, None)]
        return [(-step, self.z >= step), (step, self.z + step < self.deep)]

    def layer(self, order):
        picked = self.z
        for z in range(self.deep):
            ranked = sorted(range(self.deep), key=lambda other: (abs(other - z), other))
            picked = jnp.where(self.z == z, ranked[order], picked)
        return picked


def when(cond, act):
    if cond is None:
        act()
    else:
        pl.when(cond)(act)


def both(a, b):
    return b if a is None else jnp.logical_and(a, b)


def greet(me):
    barrier = pltpu.get_barrier_semaphore()
    partners = [
        (None, me.at(0, (1, 0)), me.c),
        (None, me.at(0, (0, 1)), me.c),
        (None, me.g, 1 - me.c),
        (me.below, me.at(-1), me.c),
        (me.above, me.at(1), me.c),
    ]
    for cond, g, c in partners:
        when(cond, lambda g=g, c=c: pl.semaphore_signal(
            barrier, inc=1, device_id=(g, c), device_id_type=MESH))
    edges = (me.z > 0).astype(jnp.int32) + (me.z < me.deep - 1).astype(jnp.int32)
    pl.semaphore_wait(barrier, 3 + edges)


def layer_kernel(columns, split, tiles, tokens_hbm, ids_ref, gains_ref, wg_hbm, wu_hbm, wd_hbm, out_ref,
                 rows_ref, wg, wu, wd, hid, part, mine, two, one, low, high,
                 own_sem, weight_sem, gz_send, gz_ici, gz_loc, gc_send, gc_ici, gc_half, gc_loc,
                 sl_send, sl_recv, sz_send, two_sem, one_sem, low_sem, high_sem,
                 sc_send, sx_send, xtwo_sem, xone_sem, clow_sem, chigh_sem):
    me = Place(columns)
    deep = me.deep
    rows, width = tokens_hbm.shape
    half = rows // 2
    lot = 8 * rows
    experts, _, units = wd.shape
    blocks = units // TILE
    lines = [me.line(step) for step in range(deep)]
    layers = [me.layer(order) for order in range(deep)]
    front, rest = slice(0, split), slice(split, width)
    carried = slice(split, rows_ref.shape[1])
    spots = (HERE,) + FLIPS + (DIAG,)
    sends = []

    own_rows = pl.multiple_of((me.z * 8 + me.c * 4 + me.spot(HERE)) * rows, rows)
    own_copy = pltpu.make_async_copy(
        tokens_hbm, rows_ref.at[pl.ds(own_rows, rows), 0:width], own_sem)
    own_copy.start()
    weight_copies = []
    for s in range(experts * blocks):
        e, n = divmod(s, blocks)
        for kind, (source, target) in enumerate(((wg_hbm, wg), (wu_hbm, wu))):
            weight_copies.append(pltpu.make_async_copy(
                source.at[e, :, n * TILE:(n + 1) * TILE], target.at[s], weight_sem.at[kind, s]))
    for e in range(experts):
        weight_copies.append(pltpu.make_async_copy(wd_hbm.at[e], wd.at[e], weight_sem.at[2, e]))
    for copy in weight_copies:
        copy.start()
    numbers = lax.broadcasted_iota(jnp.int32, (rows, rows_ref.shape[1] - width), 1)
    table = jnp.zeros(numbers.shape, jnp.float32)
    gains = gains_ref[...].astype(jnp.float32)
    ids = ids_ref[...]
    for k in range(ids.shape[1]):
        table = table + jnp.where(ids[:, k:k + 1] == numbers, gains[:, k:k + 1], 0.0)
    rows_ref[pl.ds(own_rows, rows), width:] = table.astype(rows_ref.dtype)
    greet(me)

    def row(c, dz=0, flip=HERE, h=0):
        return pl.multiple_of(((me.z + dz) * 8 + c * 4 + me.spot(flip)) * rows + h * half, half)

    def post(dz=0, flip=HERE, h=0):
        return pl.multiple_of(((me.z + dz) * 4 + me.spot(flip)) * rows + h * half, half)

    def device(kind, h=0):
        return {
            "up": lambda: (me.at(1), me.c),
            "down": lambda: (me.at(-1), me.c),
            "near": lambda: (me.at(0, FLIPS[h]), me.c),
            "side": lambda: (me.at(0, FLIPS[1 - h]), me.c),
            "core": lambda: (me.g, 1 - me.c),
        }[kind]()

    def remote(source, target, send_sem, recv_sem, where):
        return pltpu.make_async_remote_copy(
            src_ref=source, dst_ref=target, send_sem=send_sem, recv_sem=recv_sem,
            device_id=where, device_id_type=MESH)

    def issue(cond, make):
        when(cond(), lambda: make().start())
        sends.append((cond, make))

    def landed(ref, sem):
        remote(ref, ref, own_sem, sem, (me.g, 1 - me.c)).wait_recv()

    ALWAYS = lambda: None
    SLOT = {"up": 0, "down": 1, "near": 2, "side": 3, "core": 4}

    def z_slot(h, dz, flip):
        return rows_ref.at[pl.ds(row(me.c, dz, flip, h), half), carried]

    def push_z(cond, h, dz, flip, kind):
        def make():
            g = me.at(dz, flip)
            slot = z_slot(h, dz, flip)
            recv = gz_loc if kind == "core" else gz_ici
            return remote(slot, slot, gz_send.at[h, g, SLOT[kind]], recv.at[h, g], device(kind, h))
        issue(cond, make)

    def z_landed(cond, h, dz, flip):
        when(cond, lambda: landed(z_slot(h, dz, flip), gz_ici.at[h, me.at(dz, flip)]))

    def c_slot(dz, flip, h=None):
        size = rows if h is None else half
        return rows_ref.at[pl.ds(row(me.c, dz, flip, h or 0), size), front]

    def push_c(cond, dz, flip, kind, h=None, k=0):
        def make():
            g = me.at(dz, flip)
            slot = c_slot(dz, flip, h)
            recv = gc_loc.at[g] if kind == "core" else gc_ici.at[g] if h is None else gc_half.at[h]
            return remote(slot, slot, gc_send.at[g, SLOT[kind]], recv, device(kind, k))
        issue(cond, make)

    def z_first(step):
        for dz, cond in lines[step]:
            for h in range(2):
                if step:
                    z_landed(cond, h, dz, HERE)
                if dz <= 0:
                    push_z(lambda cond=cond: both(cond, me.above), h, dz, HERE, "up")
                if dz >= 0:
                    push_z(lambda cond=cond: both(cond, me.below), h, dz, HERE, "down")
                push_z(lambda cond=cond: cond, h, dz, HERE, "near")
            for h in range(2):
                push_z(lambda cond=cond: cond, h, dz, HERE, "side")
                push_z(lambda cond=cond: cond, h, dz, HERE, "core")

    def z_second(step):
        for dz, cond in lines[step]:
            for h in range(2):
                z_landed(cond, h, dz, FLIPS[h])
                push_z(lambda cond=cond: cond, h, dz, FLIPS[h], "side")
                push_z(lambda cond=cond: cond, h, dz, FLIPS[h], "core")

    def z_third(step):
        for dz, cond in lines[step]:
            for h in range(2):
                for flip in (FLIPS[1 - h], DIAG):
                    z_landed(cond, h, dz, flip)
                    push_z(lambda cond=cond: cond, h, dz, flip, "core")

    def along(flip):
        push_c(lambda: me.above, 0, flip, "up")
        push_c(lambda: me.below, 0, flip, "down")
        push_c(ALWAYS, 0, flip, "core")

    def c_first():
        for k in range(2):
            push_c(ALWAYS, 0, HERE, "near" if k == 0 else "side")
        along(HERE)

    def c_second():
        for k in range(2):
            landed(c_slot(0, FLIPS[k]), gc_ici.at[me.at(0, FLIPS[k])])
            push_c(ALWAYS, 0, FLIPS[k], "side", h=k, k=k)
            along(FLIPS[k])

    def c_third():
        for h in range(2):
            landed(c_slot(0, DIAG, h), gc_half.at[h])
        along(DIAG)

    def c_line(step):
        for dz, cond in lines[step]:
            for flip in spots:
                when(cond, lambda: landed(c_slot(dz, flip), gc_ici.at[me.at(dz, flip)]))
                if dz < 0:
                    push_c(lambda cond=cond: both(cond, me.above), dz, flip, "up")
                else:
                    push_c(lambda cond=cond: both(cond, me.below), dz, flip, "down")
                push_c(lambda cond=cond: cond, dz, flip, "core")

    def other_core(order):
        for spot in range(4):
            g = layers[order] * 4 + spot
            base = pl.multiple_of((layers[order] * 8 + (1 - me.c) * 4 + spot) * rows, rows)
            landed(rows_ref.at[pl.ds(base, rows), front], gc_loc.at[g])
            for h in range(2):
                start = pl.multiple_of(base + h * half, half)
                landed(rows_ref.at[pl.ds(start, half), carried], gz_loc.at[h, g])

    def hidden_step(order, s):
        base = pl.multiple_of(layers[order] * lot, lot)
        e, n = lax.div(s, blocks), lax.rem(s, blocks)
        x = rows_ref[pl.ds(base, lot), 0:width]
        gate = jnp.dot(x, wg[s], preferred_element_type=jnp.float32)
        upward = jnp.dot(x, wu[s], preferred_element_type=jnp.float32)
        scales = rows_ref[pl.ds(base, lot), width:].astype(jnp.float32)
        lane = lax.broadcasted_iota(jnp.int32, scales.shape, 1)
        scale = jnp.sum(jnp.where(lane == me.g * experts + e, scales, 0.0), axis=1, keepdims=True)
        value = jax.nn.silu(gate) * upward * scale
        hid[e, :, pl.ds(pl.multiple_of(n * TILE, TILE), TILE)] = value.astype(hid.dtype)

    def down_step(order, t):
        base = pl.multiple_of(layers[order] * lot, lot)
        cols = slice(*tiles[t])
        total = None
        for e in range(experts):
            term = lax.dot_general(
                hid[e], wd[e, cols, :], (((1,), (1,)), ((), ())), preferred_element_type=jnp.float32)
            total = term if total is None else total + term
        part[pl.ds(base, lot), cols] = total.astype(part.dtype)

        def make():
            start = pl.multiple_of((layers[order] * 8 + (1 - me.c) * 4) * rows, 4 * rows)
            there = pl.multiple_of(layers[order] * 4 * rows, 4 * rows)
            return remote(
                part.at[pl.ds(start, 4 * rows), cols], mine.at[pl.ds(there, 4 * rows), cols],
                sl_send.at[layers[order], t], sl_recv.at[layers[order], t], device("core"))
        issue(ALWAYS, make)

    def add(size, cols, terms, target, start):
        for at in range(cols.start, cols.stop, TILE):
            piece = slice(at, at + TILE)
            total = None
            for ref, base in terms:
                term = ref[pl.ds(base, size), piece].astype(jnp.float32)
                total = term if total is None else total + term
            target[pl.ds(start, size), piece] = total.astype(target.dtype)

    def own_terms(dz, flip, h=0):
        return [(part, row(me.c, dz, flip, h)), (mine, post(dz, flip, h))]

    def from_core(dz, steps):
        start = pl.multiple_of((me.z + dz) * 4 * rows, 4 * rows)
        for t in steps:
            landed(mine.at[pl.ds(start, 4 * rows), slice(*tiles[t])], sl_recv.at[me.z + dz, t])

    def two_at(dz, j, h):
        return pl.multiple_of((((me.z + dz) * 2 + j) * 2 + h) * half, half)

    def one_at(dz, h):
        return pl.multiple_of(((me.z + dz) * 2 + h) * half, half)

    def send_sum(cond, dz, flip, h, size, cols, target, there, send_sem, recv_sem, kind):
        def make():
            return remote(
                mine.at[pl.ds(post(dz, flip, h), size), cols],
                target.at[pl.ds(there(), size), cols], send_sem(), recv_sem(), device(kind, h))
        issue(cond, make)

    def s_third(step):
        for dz, cond in lines[step]:
            when(cond, lambda: from_core(dz, range(1, len(tiles))))
            for h in range(2):
                for j, flip in ((1, DIAG), (0, FLIPS[1 - h])):
                    when(cond, lambda: add(
                        half, rest, own_terms(dz, flip, h), mine, post(dz, flip, h)))
                    send_sum(
                        lambda cond=cond: cond, dz, flip, h, half, rest, two,
                        lambda dz=dz, j=j, h=h: two_at(dz, j, h),
                        lambda dz=dz, flip=flip, h=h: sz_send.at[h, me.at(dz, flip)],
                        lambda dz=dz, j=j, h=h: two_sem.at[me.z + dz, j, h], "side")

    def s_second(step):
        for dz, cond in lines[step]:
            for h in range(2):
                flip = FLIPS[h]

                def act():
                    landed(two.at[pl.ds(two_at(dz, 1, h), half), rest], two_sem.at[me.z + dz, 1, h])
                    add(half, rest, own_terms(dz, flip, h) + [(two, two_at(dz, 1, h))],
                        mine, post(dz, flip, h))
                when(cond, act)
                send_sum(
                    lambda cond=cond: cond, dz, flip, h, half, rest, one,
                    lambda dz=dz, h=h: one_at(dz, h),
                    lambda dz=dz, flip=flip, h=h: sz_send.at[h, me.at(dz, flip)],
                    lambda dz=dz, h=h: one_sem.at[me.z + dz, h], "near")

    def from_line(ref, sem, edge, dz, h):
        at = ref.at[pl.ds(post(dz, HERE, h), half), rest]
        pl.when(edge)(lambda: landed(at, sem.at[me.z + dz, h]))

    def s_first(step):
        for dz, cond in lines[step]:
            for h in range(2):
                def act():
                    landed(two.at[pl.ds(two_at(dz, 0, h), half), rest], two_sem.at[me.z + dz, 0, h])
                    landed(one.at[pl.ds(one_at(dz, h), half), rest], one_sem.at[me.z + dz, h])
                    terms = own_terms(dz, HERE, h) + [(two, two_at(dz, 0, h)), (one, one_at(dz, h))]
                    if dz >= 0:
                        from_line(low, low_sem, me.below, dz, h)
                        terms.append((low, post(dz, HERE, h)))
                    if dz <= 0:
                        from_line(high, high_sem, me.above, dz, h)
                        terms.append((high, post(dz, HERE, h)))
                    if dz == 0:
                        add(half, rest, terms, out_ref, h * half)
                    else:
                        add(half, rest, terms, mine, post(dz, HERE, h))
                when(cond, act)
                if dz:
                    target, sem, kind = (low, low_sem, "up") if dz > 0 else (high, high_sem, "down")
                    send_sum(
                        lambda cond=cond: cond, dz, HERE, h, half, rest, target,
                        lambda dz=dz, h=h: post(dz, HERE, h),
                        lambda dz=dz, h=h: sz_send.at[h, me.at(dz)],
                        lambda dz=dz, h=h, sem=sem: sem.at[me.z + dz, h], kind)

    def c_near(dz, flip):
        g = me.at(dz, flip)
        spot = pl.ds(post(dz, flip), rows)
        if dz >= 0:
            pl.when(me.below)(lambda: landed(low.at[spot, front], clow_sem.at[g]))
        if dz <= 0:
            pl.when(me.above)(lambda: landed(high.at[spot, front], chigh_sem.at[g]))

    def t_line(step):
        for dz, cond in lines[step]:
            when(cond, lambda: from_core(dz, (0,)))
            near, sem, kind = (low, clow_sem, "up") if dz > 0 else (high, chigh_sem, "down")
            for flip in spots:
                def act():
                    c_near(dz, flip)
                    add(rows, front, own_terms(dz, flip) + [(near, post(dz, flip))],
                        mine, post(dz, flip))
                when(cond, act)
                send_sum(
                    lambda cond=cond: cond, dz, flip, 0, rows, front, near,
                    lambda dz=dz, flip=flip: post(dz, flip),
                    lambda dz=dz, flip=flip: sc_send.at[me.at(dz, flip)],
                    lambda dz=dz, flip=flip, sem=sem: sem.at[me.at(dz, flip)], kind)

    def lined(flip, h):
        return own_terms(0, flip, h) + [(low, post(0, flip, h)), (high, post(0, flip, h))]

    def t_third():
        from_core(0, (0,))
        for flip in (DIAG,) + FLIPS + (HERE,):
            c_near(0, flip)
        for h in range(2):
            for j, flip in ((1, DIAG), (0, FLIPS[1 - h])):
                add(half, front, lined(flip, h), mine, post(0, flip, h))
                send_sum(
                    ALWAYS, 0, flip, h, half, front, two, lambda j=j, h=h: two_at(0, j, h),
                    lambda j=j, h=h: sx_send.at[h, j], lambda j=j, h=h: xtwo_sem.at[j, h], "side")

    def t_second():
        for h in range(2):
            flip = FLIPS[h]
            landed(two.at[pl.ds(two_at(0, 1, h), half), front], xtwo_sem.at[1, h])
            add(half, front, lined(flip, h) + [(two, two_at(0, 1, h))], mine, post(0, flip, h))
            send_sum(
                ALWAYS, 0, flip, h, half, front, one, lambda h=h: one_at(0, h),
                lambda h=h: sx_send.at[h, 2], lambda h=h: xone_sem.at[h], "near")

    def t_first():
        for h in range(2):
            landed(two.at[pl.ds(two_at(0, 0, h), half), front], xtwo_sem.at[0, h])
            landed(one.at[pl.ds(one_at(0, h), half), front], xone_sem.at[h])
            add(half, front, lined(HERE, h) + [(two, two_at(0, 0, h)), (one, one_at(0, h))],
                out_ref, h * half)

    def clear(ref):
        def body(i, carry):
            ref[pl.ds(pl.multiple_of(i * half, half), half), :] = jnp.zeros((half, width), ref.dtype)
            return carry
        lax.fori_loop(0, ref.shape[0] // half, body, None)

    last = deep - 1
    own_copy.wait()
    c_first()
    z_first(0)
    c_second()
    pl.when(jnp.logical_not(me.below))(lambda: clear(low))
    pl.when(jnp.logical_not(me.above))(lambda: clear(high))
    gather_steps = gather_plan(deep, dict(
        z_first=z_first, z_second=z_second, z_third=z_third, c_third=c_third, c_line=c_line))
    run(gather_steps[0])
    for copy in weight_copies:
        copy.wait()
    subs = experts * blocks
    for order in range(deep):
        other_core(order)
        acts = gather_steps[1 + order]

        def body(s, carry, order=order, acts=acts):
            for k in range(subs):
                if acts[k]:
                    pl.when(s == k)(lambda k=k: run(acts[k]))
            hidden_step(order, s)
            return carry
        lax.fori_loop(0, subs, body, None)
        for t in range(len(tiles)):
            down_step(order, t)
            if subs + t < len(acts):
                run(acts[subs + t])
    for turn in range(deep + 2):
        for stage, lag in ((s_third, 0), (s_second, 1), (s_first, 2)):
            if 0 <= turn - lag < deep:
                stage(last - (turn - lag))
        if turn < last:
            t_line(last - turn)
        elif turn < deep + 2:
            (t_third, t_second, t_first)[turn - last]()
    for cond, make in sends:
        when(cond(), lambda: make().wait_send())


def run(acts):
    for act in acts:
        act()


def gather_plan(deep, do):
    def act(name, *args):
        return lambda: do[name](*args) if not args or args[0] < deep else None
    before = [act("z_second", 0), act("z_first", 1), act("c_third"), act("z_third", 0)]
    plan = [[[] for _ in range(8)] for _ in range(deep)]
    for order in range(deep):
        step = order + 1
        plan[order][0] += [act("z_second", step), act("c_line", step)]
        plan[order][1] += [act("z_first", step + 1)]
        plan[order][3] += [act("z_third", step)]
    return [before] + plan


def fused_body(tokens, gate_weights, expert_ids, w_gate, w_up, w_down):
    columns = lax.axis_size("grp")
    rows, width = tokens.shape
    experts, _, units = w_gate.shape
    deep = columns // 4
    half = rows // 2
    split = max(1, round(width * 2 / 9 / TILE)) * TILE
    edges = list(range(split, width, 4 * TILE)) + [width]
    tiles = [(0, split)] + list(zip(edges[:-1], edges[1:]))
    padded = -(-columns * experts // LANES) * LANES
    blocks = units // TILE
    bf16 = tokens.dtype
    dma = pltpu.SemaphoreType.DMA
    vmem = lambda *shape: pltpu.VMEM(shape, bf16)
    anywhere = pl.BlockSpec(memory_space=pl.ANY)
    local = pl.BlockSpec(memory_space=pltpu.VMEM)
    lined = columns * rows
    return pl.pallas_call(
        functools.partial(layer_kernel, columns, split, tiles),
        out_shape=jax.ShapeDtypeStruct((rows, width), bf16),
        in_specs=[anywhere, local, local, anywhere, anywhere, anywhere],
        out_specs=local,
        scratch_shapes=[
            vmem(2 * lined, width + padded),
            vmem(experts * blocks, width, TILE), vmem(experts * blocks, width, TILE),
            vmem(experts, width, units),
            vmem(experts, 8 * rows, units),
            vmem(2 * lined, width), vmem(lined, width),
            vmem(deep * 4 * half, width), vmem(deep * rows, width),
            vmem(lined, width), vmem(lined, width),
            dma, dma((3, experts * blocks)),
            dma((2, columns, 5)), dma((2, columns)), dma((2, columns)),
            dma((columns, 5)), dma((columns,)), dma((2,)), dma((columns,)),
            dma((deep, len(tiles))), dma((deep, len(tiles))),
            dma((2, columns)), dma((deep, 2, 2)), dma((deep, 2)), dma((deep, 2)), dma((deep, 2)),
            dma((columns,)), dma((2, 3)), dma((2, 2)), dma((2,)), dma((columns,)), dma((columns,)),
        ],
        compiler_params=pltpu.CompilerParams(
            collective_id=1, has_side_effects=True, vmem_limit_bytes=60 * 2**20),
        name="expert_layer",
    )(tokens, expert_ids, gate_weights, w_gate, w_up, w_down)


def expert_rows(inputs, scales, gate_part, up_part, down_part):
    gate_act = jnp.dot(inputs, gate_part, preferred_element_type=jnp.float32)
    upward = jnp.dot(inputs, up_part, preferred_element_type=jnp.float32)
    hidden = (jax.nn.silu(gate_act) * upward).astype(jnp.bfloat16)
    projected = lax.dot_general(
        hidden, down_part, (((1,), (1,)), ((), ())), preferred_element_type=jnp.float32
    )
    return projected * scales.astype(jnp.float32)[:, None]


def weights_path(rows_in, scales_in, w_gate, w_up, w_down):
    row_dims = rows_in.shape
    shard_units = w_gate.shape[2]
    expert_inputs = [rows_in[:, expert].reshape(-1, row_dims[3]) for expert in range(row_dims[1])]
    expert_scales = [scales_in[:, expert].reshape(-1) for expert in range(row_dims[1])]
    starting = tuple(
        (
            jnp.zeros((row_dims[0] * row_dims[2], row_dims[3]), jnp.float32)
            for expert in range(row_dims[1])
        )
    )
    gate_piece = lax.all_gather(w_gate, "loc", axis=2, tiled=True)
    up_piece = lax.all_gather(w_up, "loc", axis=2, tiled=True)
    down_piece = lax.all_gather(w_down, "loc", axis=2, tiled=True)
    updated = []
    for expert in range(row_dims[1]):
        running = starting[expert]
        for block_index in range(gate_piece.shape[2] // shard_units):
            lower_unit = block_index * shard_units
            upper_unit = lower_unit + shard_units
            values = expert_rows(
                expert_inputs[expert],
                expert_scales[expert],
                gate_piece[expert][:, lower_unit:upper_unit],
                up_piece[expert][:, lower_unit:upper_unit],
                down_piece[expert][:, lower_unit:upper_unit],
            )
            rounded = lax.optimization_barrier(values.astype(jnp.bfloat16))
            running = running + rounded.astype(jnp.float32)
        updated.append(running)
    folded = tuple(updated)
    stacked = jnp.stack(
        [folded_part.reshape(row_dims[0], row_dims[2], row_dims[3]) for folded_part in folded],
        axis=1,
    )
    return stacked.astype(jnp.bfloat16)


def slot_body(tokens, gate_weights, expert_ids, w_gate, w_up, w_down):
    tok_count = tokens.shape[0]
    choices_per = expert_ids.shape[1]
    feature_count = tokens.shape[1]
    group_count = lax.axis_size("grp")
    local_experts = w_gate.shape[0]
    expert_total = group_count * local_experts
    slot_depth = 2 * tok_count * RGROUPS // expert_total
    slot_total = expert_total * slot_depth
    pair_ids = expert_ids.reshape(-1)
    pair_count = pair_ids.shape[0]
    pair_order = jnp.arange(pair_count, dtype=jnp.int32)
    same_expert = (pair_ids[:, None] == pair_ids[None, :]).astype(jnp.int32)
    earlier = (pair_order[:, None] > pair_order[None, :]).astype(jnp.int32)
    slot_rank = jnp.sum(same_expert * earlier, axis=1)
    position = pair_ids * slot_depth + slot_rank
    pair_onehot = jnp.arange(slot_total, dtype=jnp.int32)[:, None] == position[None, :]
    placement = jnp.sum(
        pair_onehot.reshape(slot_total, tok_count, choices_per).astype(jnp.int32), axis=2
    ).astype(jnp.bfloat16)
    send_rows = jnp.dot(placement, tokens, preferred_element_type=jnp.float32).astype(jnp.bfloat16)
    flat_scales = gate_weights.reshape(-1).astype(jnp.float32)
    send_scales = jnp.sum(jnp.where(pair_onehot, flat_scales[None, :], 0.0), axis=1).astype(
        jnp.bfloat16
    )
    send_rows = send_rows.reshape(group_count, local_experts, slot_depth, feature_count)
    send_scales = send_scales.reshape(group_count, local_experts, slot_depth)
    computed = weights_path(
        lax.all_to_all(send_rows, "grp", split_axis=0, concat_axis=0, tiled=True),
        lax.all_to_all(send_scales, "grp", split_axis=0, concat_axis=0, tiled=True),
        w_gate,
        w_up,
        w_down,
    )
    returned = lax.all_to_all(computed, "grp", split_axis=0, concat_axis=0, tiled=True)
    flat_back = returned.reshape(slot_total, feature_count)
    mixed_out = lax.dot_general(
        placement, flat_back, (((0,), (0,)), ((), ())), preferred_element_type=jnp.float32
    )
    return mixed_out.astype(jnp.bfloat16)


def body(tokens, gate_weights, expert_ids, w_gate, w_up, w_down):
    tok_count, width = tokens.shape
    units = w_gate.shape[2]
    columns = lax.axis_size("grp")
    slot_depth = 2 * tok_count * RGROUPS // (columns * w_gate.shape[0])
    dense = slot_depth * w_gate.shape[0] >= tok_count
    fits = (columns % 4 == 0 and lax.axis_size("loc") == 2 and tok_count % 32 == 0
            and width % TILE == 0 and width > TILE and units % TILE == 0)
    chosen = fused_body if dense and fits else slot_body
    return chosen(tokens, gate_weights, expert_ids, w_gate, w_up, w_down)


def solution(mesh):
    placed = (
        P(("grp", "loc"), None),
        P(("grp", "loc"), None),
        P(("grp", "loc"), None),
        P("grp", None, "loc"),
        P("grp", None, "loc"),
        P("grp", None, "loc"),
    )
    return jax.shard_map(
        body, mesh=mesh, in_specs=placed, out_specs=P(("grp", "loc"), None), check_vma=False
    )
```

```python
import functools

import jax
import jax.numpy as jnp
from jax import lax
from jax.experimental import pallas as pl
from jax.experimental.pallas import tpu as pltpu
from jax.sharding import PartitionSpec as P

RGROUPS = 8
LANES = 128
TILE = 256
MESH = pl.DeviceIdType.MESH
FLIPS = ((1, 0), (0, 1))
HERE, DIAG = (0, 0), (1, 1)


class Place:
    def __init__(self, columns):
        self.deep = columns // 4
        self.g = lax.axis_index("grp")
        self.c = lax.axis_index("loc")
        self.x = lax.rem(self.g, 2)
        self.y = lax.rem(lax.div(self.g, 2), 2)
        self.z = lax.div(self.g, 4)
        self.below = self.z > 0
        self.above = self.z < self.deep - 1
        self.end = jnp.logical_or(self.z == 0, self.z == self.deep - 1)

    def spot(self, flip):
        x = 1 - self.x if flip[0] else self.x
        y = 1 - self.y if flip[1] else self.y
        return y * 2 + x

    def at(self, dz=0, flip=HERE):
        return (self.z + dz) * 4 + self.spot(flip)

    def line(self, step):
        if step == 0:
            return [(0, None)]
        return [(-step, self.z >= step), (step, self.z + step < self.deep)]

    def layer(self, order):
        picked = self.z
        for z in range(self.deep):
            ranked = sorted(range(self.deep), key=lambda other: (abs(other - z), other))
            picked = jnp.where(self.z == z, ranked[order], picked)
        return picked


def when(cond, act):
    if cond is None:
        act()
    else:
        pl.when(cond)(act)


def both(a, b):
    return b if a is None else jnp.logical_and(a, b)


def greet(me):
    barrier = pltpu.get_barrier_semaphore()
    partners = [
        (None, me.at(0, (1, 0)), me.c),
        (None, me.at(0, (0, 1)), me.c),
        (None, me.g, 1 - me.c),
        (me.below, me.at(-1), me.c),
        (me.above, me.at(1), me.c),
    ]
    for cond, g, c in partners:
        when(cond, lambda g=g, c=c: pl.semaphore_signal(
            barrier, inc=1, device_id=(g, c), device_id_type=MESH))
    edges = (me.z > 0).astype(jnp.int32) + (me.z < me.deep - 1).astype(jnp.int32)
    pl.semaphore_wait(barrier, 3 + edges)


def layer_kernel(columns, split, tiles, tokens_hbm, ids_ref, gains_ref, wg_hbm, wu_hbm, wd_hbm, out_ref,
                 rows_ref, wg, wu, wd, hid, part, mine, two, one, low, high,
                 far, own_sem, weight_sem, down_sem, send_sem, gz_ici, gc_ici, gc_half, core_sem,
                 sum_sem, two_sem, one_sem, low_sem, high_sem, far_sem,
                 xtwo_sem, xone_sem, clow_sem, chigh_sem, cfar_sem):
    me = Place(columns)
    deep = me.deep
    rows, width = tokens_hbm.shape
    half = rows // 2
    lot = 8 * rows
    experts, _, units = wd_hbm.shape
    blocks = units // TILE
    lines = [me.line(step) for step in range(deep)]
    layers = [me.layer(order) for order in range(deep)]
    at_layer = [me.z == layer for layer in range(deep)]
    front, rest = slice(0, split), slice(split, width)
    carried = slice(split, rows_ref.shape[1])
    spots = (HERE,) + FLIPS + (DIAG,)
    sends = {}
    last = deep - 1
    jump = deep > 2

    own_rows = pl.multiple_of((me.z * 8 + me.c * 4 + me.spot(HERE)) * rows, rows)
    own_copy = pltpu.make_async_copy(
        tokens_hbm, rows_ref.at[pl.ds(own_rows, rows), 0:width], own_sem)
    own_copy.start()

    def weights():
        for e in range(experts):
            for b in range(width // units):
                pltpu.make_async_copy(
                    wd_hbm.at[e, b * units:(b + 1) * units, :],
                    wd.at[e * units:(e + 1) * units, b * units:(b + 1) * units], down_sem.at[e]).start()
        for s in range(experts * blocks):
            e, n = divmod(s, blocks)
            for kind, (source, target) in enumerate(((wg_hbm, wg), (wu_hbm, wu))):
                pltpu.make_async_copy(
                    source.at[e, :, n * TILE:(n + 1) * TILE], target.at[s], weight_sem.at[kind]).start()

    numbers = lax.broadcasted_iota(jnp.int32, (rows_ref.shape[1] - width, rows), 0)
    table = jnp.zeros(numbers.shape, jnp.float32)
    gains = gains_ref[...].astype(jnp.float32)
    ids = ids_ref[...]
    for k in range(ids.shape[0]):
        table = table + jnp.where(ids[k:k + 1, :] == numbers, gains[k:k + 1, :], 0.0)
    table = table.astype(rows_ref.dtype)
    unit = (lax.broadcasted_iota(jnp.int32, (rows, rows), 0)
            == lax.broadcasted_iota(jnp.int32, (rows, rows), 1)).astype(rows_ref.dtype)
    rows_ref[pl.ds(own_rows, rows), width:] = lax.dot_general(
        unit, table, (((1,), (1,)), ((), ())), preferred_element_type=jnp.float32).astype(rows_ref.dtype)
    greet(me)

    def row(c, layer, flip=HERE, h=0):
        return pl.multiple_of((layer * 8 + c * 4 + me.spot(flip)) * rows + h * half, half)

    def post(layer, flip=HERE, h=0):
        return pl.multiple_of((layer * 4 + me.spot(flip)) * rows + h * half, half)

    def column(layer, flip=HERE):
        return layer * 4 + me.spot(flip)

    def device(kind, h=0):
        return {
            "up": lambda: (me.at(1), me.c),
            "down": lambda: (me.at(-1), me.c),
            "near": lambda: (me.at(0, FLIPS[h]), me.c),
            "side": lambda: (me.at(0, FLIPS[1 - h]), me.c),
            "core": lambda: (me.g, 1 - me.c),
        }[kind]()

    def remote(source, target, send_sem, recv_sem, where):
        return pltpu.make_async_remote_copy(
            src_ref=source, dst_ref=target, send_sem=send_sem, recv_sem=recv_sem,
            device_id=where, device_id_type=MESH)

    def issue(key, cond, size, cols, make):
        number, _, total, _ = sends.get(key, (len(sends), cond, 0, cols))
        sends[key] = (number, cond, total + size, cols)
        when(cond(), lambda: make(send_sem.at[number]).start())

    def landed(ref, sem):
        remote(ref, ref, own_sem, sem, (me.g, 1 - me.c)).wait_recv()

    def always():
        return None

    def z_slot(h, layer, flip):
        return rows_ref.at[pl.ds(row(me.c, layer, flip, h), half), carried]

    def push_z(key, cond, h, layer, flip, kind):
        def make(sem):
            slot = z_slot(h, layer(), flip)
            recv = core_sem.at[layer()] if kind == "core" else gz_ici.at[h, column(layer(), flip)]
            return remote(slot, slot, sem, recv, device(kind, h))
        issue(key, cond, half, carried, make)

    def z_landed(h, layer, flip):
        landed(z_slot(h, layer, flip), gz_ici.at[h, column(layer, flip)])

    def c_slot(layer, flip, h=None):
        size = rows if h is None else half
        return rows_ref.at[pl.ds(row(me.c, layer, flip, h or 0), size), front]

    def push_c(key, cond, layer, flip, kind, h=None, k=0):
        size = rows if h is None else half

        def make(sem):
            slot = c_slot(layer(), flip, h)
            recv = (core_sem.at[layer()] if kind == "core"
                    else gc_ici.at[column(layer(), flip)] if h is None else gc_half.at[h])
            return remote(slot, slot, sem, recv, device(kind, k))
        issue(key, cond, size, front, make)

    def z_first(step):
        for dz, cond in lines[step]:
            layer = lambda dz=dz: me.z + dz
            for h in range(2):
                if step:
                    when(cond, lambda: z_landed(h, layer(), HERE))
                if dz <= 0 and step < last:
                    push_z(("up", dz), lambda cond=cond: both(cond, me.above), h, layer, HERE, "up")
                if dz >= 0 and step < last:
                    push_z(("down", dz), lambda cond=cond: both(cond, me.below), h, layer, HERE, "down")

    def z_cross(order):
        for kind in ("near", "side", "core"):
            for h in range(2):
                push_z(("cross", order), always, h, lambda: layers[order], HERE, kind)

    def z_second(order):
        for h in range(2):
            z_landed(h, layers[order], FLIPS[h])
            push_z(("second", order), always, h, lambda: layers[order], FLIPS[h], "side")
            push_z(("second", order), always, h, lambda: layers[order], FLIPS[h], "core")

    def z_third(order):
        for flips in (lambda h: FLIPS[1 - h], lambda h: DIAG):
            for h in range(2):
                z_landed(h, layers[order], flips(h))
                push_z(("third", order), always, h, lambda: layers[order], flips(h), "core")

    def own():
        return me.z

    def along(flip):
        push_c("c up", lambda: me.above, own, flip, "up")
        push_c("c down", lambda: me.below, own, flip, "down")
        push_c("c core", always, own, flip, "core")

    def c_first():
        for k in range(2):
            push_c("c first", always, own, HERE, "near" if k == 0 else "side")
        along(HERE)

    def c_second():
        for k in range(2):
            landed(c_slot(me.z, FLIPS[k]), gc_ici.at[me.at(0, FLIPS[k])])
            push_c("c second", always, own, FLIPS[k], "side", h=k, k=k)
            along(FLIPS[k])

    def c_third():
        for h in range(2):
            landed(c_slot(me.z, DIAG, h), gc_half.at[h])
        along(DIAG)

    def c_line(step):
        for dz, cond in lines[step]:
            layer = lambda dz=dz: me.z + dz
            for flip in spots:
                when(cond, lambda: landed(c_slot(layer(), flip), gc_ici.at[column(layer(), flip)]))
                if step < last:
                    edge, kind = (me.above, "up") if dz < 0 else (me.below, "down")
                    push_c(("c on", dz), lambda cond=cond, edge=edge: both(cond, edge), layer, flip, kind)
                push_c(("c in", dz), lambda cond=cond: cond, layer, flip, "core")

    def other_core(order):
        base = pl.multiple_of((layers[order] * 8 + (1 - me.c) * 4) * rows, 4 * rows)
        landed(rows_ref.at[pl.ds(base, 4 * rows), :], core_sem.at[layers[order]])

    def turn_down(e):
        whole = wd.at[e * units:(e + 1) * units, :]
        pltpu.make_async_copy(whole, whole, down_sem.at[e]).wait()
        for b in range(width // units):
            block = (slice(e * units, (e + 1) * units), slice(b * units, (b + 1) * units))
            wd[block] = wd[block].T

    def hidden_step(order, s):
        base = pl.multiple_of(layers[order] * lot, lot)
        e = lax.div(s, blocks)
        x = rows_ref[pl.ds(base, lot), 0:width]
        gate = jnp.dot(x, wg[s], preferred_element_type=jnp.float32)
        upward = jnp.dot(x, wu[s], preferred_element_type=jnp.float32)
        scales = rows_ref[pl.ds(base, lot), width:].astype(jnp.float32)
        lane = lax.broadcasted_iota(jnp.int32, scales.shape, 1)
        scale = jnp.sum(jnp.where(lane == me.g * experts + e, scales, 0.0), axis=1, keepdims=True)
        value = jax.nn.silu(gate) * upward * scale
        hid[:, pl.ds(pl.multiple_of(s * TILE, TILE), TILE)] = value.astype(hid.dtype)

    def down_step(order, t):
        base = pl.multiple_of(layers[order] * lot, lot)
        cols = slice(*tiles[t])
        total = jnp.dot(hid[...], wd[:, cols], preferred_element_type=jnp.float32)
        part[pl.ds(base, lot), cols] = total.astype(part.dtype)

        def make(sem):
            start = pl.multiple_of((layers[order] * 8 + (1 - me.c) * 4) * rows, 4 * rows)
            there = pl.multiple_of(layers[order] * 4 * rows, 4 * rows)
            return remote(
                part.at[pl.ds(start, 4 * rows), cols], mine.at[pl.ds(there, 4 * rows), cols],
                sem, sum_sem.at[layers[order]], device("core"))
        tail = slice(0, width) if t == len(tiles) - 1 else cols
        issue(("part", order), always, 4 * rows if t == len(tiles) - 1 else 0, tail, make)

    def add(size, cols, terms, target, start):
        for at in range(cols.start, cols.stop, TILE):
            piece = slice(at, at + TILE)
            total = None
            for ref, base in terms:
                term = ref[pl.ds(base, size), piece].astype(jnp.float32)
                total = term if total is None else total + term
            target[pl.ds(start, size), piece] = total.astype(target.dtype)

    def own_terms(layer, flip, h=0):
        return [(part, row(me.c, layer, flip, h)), (mine, post(layer, flip, h))]

    def from_core(order):
        start = pl.multiple_of(layers[order] * 4 * rows, 4 * rows)
        landed(mine.at[pl.ds(start, 4 * rows), :], sum_sem.at[layers[order]])

    def two_at(layer, j, h):
        return pl.multiple_of(((layer * 2 + j) * 2 + h) * half, half)

    def one_at(layer, h):
        return pl.multiple_of((layer * 2 + h) * half, half)

    def two_slot(layer, j, h, cols):
        return two.at[pl.ds(two_at(layer, j, h), half), cols]

    def one_slot(layer, h, cols):
        return one.at[pl.ds(one_at(layer, h), half), cols]

    def send_sum(key, cond, layer, flip, h, size, cols, target, recv_sem, where):
        def make(sem):
            return remote(
                mine.at[pl.ds(post(layer(), flip, h), size), cols], target(), sem, recv_sem(), where())
        issue(key, cond, size, cols, make)

    def s_third(order):
        layer = lambda: layers[order]
        from_core(order)
        for j, flips in ((1, lambda h: DIAG), (0, lambda h: FLIPS[1 - h])):
            for h in range(2):
                flip = flips(h)
                add(half, rest, own_terms(layer(), flip, h), mine, post(layer(), flip, h))
                send_sum(
                    ("s third", order), always, layer, flip, h, half, rest,
                    lambda j=j, h=h: two_slot(layer(), j, h, rest),
                    lambda j=j, h=h: two_sem.at[layer(), j, h], lambda h=h: device("side", h))

    def s_second(order):
        layer = lambda: layers[order]
        for h in range(2):
            flip = FLIPS[h]
            landed(two_slot(layer(), 1, h, rest), two_sem.at[layer(), 1, h])
            add(half, rest, own_terms(layer(), flip, h) + [(two, two_at(layer(), 1, h))],
                mine, post(layer(), flip, h))
            send_sum(
                ("s second", order), always, layer, flip, h, half, rest,
                lambda h=h: one_slot(layer(), h, rest), lambda h=h: one_sem.at[layer(), h],
                lambda h=h: device("near", h))

    def columns_in(layer, h):
        landed(two_slot(layer, 0, h, rest), two_sem.at[layer, 0, h])
        landed(one_slot(layer, h, rest), one_sem.at[layer, h])
        return own_terms(layer, HERE, h) + [(two, two_at(layer, 0, h)), (one, one_at(layer, h))]

    def ways(reach, hop):
        for cond, to, name in (
                (at_layer[hop], reach, "up"), (at_layer[deep - 1 - hop], deep - 1 - reach, "down")):
            over = jump and reach == last and hop == 0
            joins = hop > (1 if jump and reach == last else 0)
            near, z_sem, c_sem = (low, low_sem, clow_sem) if name == "up" else (high, high_sem, chigh_sem)
            yield cond, to, name, over, joins, near, z_sem, c_sem

    def z_sum(reach, hop):
        for cond, to, name, over, joins, near, sem, _ in ways(reach, hop):
            for h in range(2):
                def act():
                    terms = columns_in(to, h)
                    if joins:
                        landed(near.at[pl.ds(post(to, HERE, h), half), rest], sem.at[to, h])
                        terms.append((near, post(to, HERE, h)))
                    add(half, rest, terms, mine, post(to, HERE, h))
                pl.when(cond)(act)

                def target(to=to, near=near, over=over, h=h):
                    ref, at = (far, post(0, HERE, h)) if over else (near, post(to, HERE, h))
                    return ref.at[pl.ds(at, half), rest]
                send_sum(
                    ("z sum", name, reach, hop), lambda cond=cond: cond, lambda to=to: to, HERE, h, half,
                    rest, target,
                    lambda to=to, sem=sem, over=over, h=h: far_sem.at[h] if over else sem.at[to, h],
                    lambda to=to, name=name, over=over: (
                        (column(to), me.c) if over else device(name)))

    def c_sum(reach, hop):
        for cond, to, name, over, joins, near, _, sem in ways(reach, hop):
            for flip in spots:
                def act():
                    terms = own_terms(to, flip)
                    if joins:
                        landed(near.at[pl.ds(post(to, flip), rows), front], sem.at[column(to, flip)])
                        terms.append((near, post(to, flip)))
                    add(rows, front, terms, mine, post(to, flip))
                pl.when(cond)(act)

                def target(to=to, near=near, over=over, flip=flip):
                    ref, at = (far, post(0, flip)) if over else (near, post(to, flip))
                    return ref.at[pl.ds(at, rows), front]
                send_sum(
                    ("c sum", name, reach, hop), lambda cond=cond: cond, lambda to=to: to, flip, 0, rows,
                    front, target,
                    lambda to=to, sem=sem, over=over, flip=flip: (
                        cfar_sem.at[me.spot(flip)] if over else sem.at[column(to, flip)]),
                    lambda to=to, name=name, over=over: (
                        (column(to), me.c) if over else device(name)))

    def lined(flip, h):
        beyond = [(low, post(me.z, flip, h)), (high, post(me.z, flip, h))]
        return own_terms(me.z, flip, h) + beyond + ([(far, post(0, flip, h))] if jump else [])

    def z_final():
        for h in range(2):
            terms = columns_in(me.z, h)[2:] + lined(HERE, h)
            spot = pl.ds(post(me.z, HERE, h), half)
            pl.when(me.below)(lambda: landed(low.at[spot, rest], low_sem.at[me.z, h]))
            pl.when(me.above)(lambda: landed(high.at[spot, rest], high_sem.at[me.z, h]))
            if jump:
                spot_far = pl.ds(post(0, HERE, h), half)
                pl.when(me.end)(lambda: landed(far.at[spot_far, rest], far_sem.at[h]))
            add(half, rest, terms, out_ref, h * half)

    def c_back():
        for flip in (DIAG,) + FLIPS + (HERE,):
            g = column(me.z, flip)
            spot = pl.ds(post(me.z, flip), rows)
            pl.when(me.below)(lambda: landed(low.at[spot, front], clow_sem.at[g]))
            pl.when(me.above)(lambda: landed(high.at[spot, front], chigh_sem.at[g]))
            if jump:
                spot_far = pl.ds(post(0, flip), rows)
                pl.when(me.end)(lambda: landed(far.at[spot_far, front], cfar_sem.at[me.spot(flip)]))
        for j, flips in ((1, lambda h: DIAG), (0, lambda h: FLIPS[1 - h])):
            for h in range(2):
                flip = flips(h)
                add(half, front, lined(flip, h), mine, post(me.z, flip, h))
                send_sum(
                    "c back", always, own, flip, h, half, front,
                    lambda j=j, h=h: two_slot(me.z, j, h, front),
                    lambda j=j, h=h: xtwo_sem.at[j, h], lambda h=h: device("side", h))

    def c_cross():
        for h in range(2):
            flip = FLIPS[h]
            landed(two_slot(me.z, 1, h, front), xtwo_sem.at[1, h])
            add(half, front, lined(flip, h) + [(two, two_at(me.z, 1, h))], mine, post(me.z, flip, h))
            send_sum(
                "c cross", always, own, flip, h, half, front, lambda h=h: one_slot(me.z, h, front),
                lambda h=h: xone_sem.at[h], lambda h=h: device("near", h))

    def c_final():
        for h in range(2):
            landed(two_slot(me.z, 0, h, front), xtwo_sem.at[0, h])
            landed(one_slot(me.z, h, front), xone_sem.at[h])
            add(half, front, lined(HERE, h) + [(two, two_at(me.z, 0, h)), (one, one_at(me.z, h))],
                out_ref, h * half)

    def clear(ref, layer):
        base = layer * 4 * rows

        def body(i, carry):
            ref[pl.ds(pl.multiple_of(base + i * half, half), half), :] = jnp.zeros((half, width), ref.dtype)
            return carry
        lax.fori_loop(0, 8, body, None)

    do = dict(
        z_first=z_first, z_cross=z_cross, z_second=z_second, z_third=z_third, c_first=c_first, c_second=c_second,
        c_third=c_third, c_line=c_line, turn_down=turn_down, s_third=s_third, s_second=s_second,
        z_sum=z_sum, c_sum=c_sum, z_final=z_final, c_back=c_back, c_cross=c_cross, c_final=c_final,
        weights=weights,
        clear_low=lambda: pl.when(jnp.logical_not(me.below))(lambda: clear(low, me.z)),
        clear_high=lambda: pl.when(jnp.logical_not(me.above))(lambda: clear(high, me.z)),
        clear_far=lambda: pl.when(jnp.logical_not(me.end))(lambda: clear(far, 0)))
    before, plan, after = order_of_work(deep, experts)

    def run(acts):
        for name, *args in acts:
            do[name](*args)

    own_copy.wait()
    run(before)
    for kind, ref in enumerate((wg, wu)):
        pltpu.make_async_copy(ref, ref, weight_sem.at[kind]).wait()
    subs = experts * blocks
    for order in range(deep):
        other_core(order)
        acts = plan[order]

        def body(s, carry, order=order, acts=acts):
            for k in range(subs):
                if acts.get(k):
                    pl.when(s == k)(lambda k=k: run(acts[k]))
            hidden_step(order, s)
            return carry
        lax.fori_loop(0, subs, body, None)
        for t in range(len(tiles)):
            run(acts.get(subs + t, []))
            down_step(order, t)
    run(after)
    assert len(sends) == send_sem.shape[0], len(sends)
    for number, cond, total, cols in sends.values():
        spent = rows_ref.at[pl.ds(0, total), cols]
        when(cond(), lambda: remote(
            spent, spent, send_sem.at[number], own_sem, (me.g, 1 - me.c)).wait_send())


def order_of_work(deep, experts):
    last = deep - 1
    before = [("c_first",), ("z_first", 0), ("z_cross", 0), ("weights",)]
    before += [("clear_low",), ("clear_high",), ("clear_far",)]
    before += [("c_second",), ("turn_down", 0)]
    before += [("z_second", 0), ("z_first", 1), ("z_cross", 1)]
    before += [("turn_down", e) for e in range(1, experts)]
    before += [("c_third",), ("z_third", 0)]
    plan = [{} for _ in range(deep)]

    def put(order, step, *acts):
        plan[min(order, last)].setdefault(step, []).extend(acts)

    put(0, 1, ("z_second", 1))
    for order in range(last):
        if order:
            put(order, 0, ("z_second", order + 1))
        if order + 2 < deep:
            put(order, 1 if order else 2, ("z_first", order + 2), ("z_cross", order + 2))
        put(order, (2, 4, 4)[order] if deep == 4 else 2, ("c_line", order + 1))
        put(order, 5, ("z_third", order + 1))
    if last > 1:
        put(last - 1, 1, ("s_third", 1), ("c_sum", 1, 0))
        put(last, 0, ("s_second", 1))
        for order in range(2, last):
            put(last, 1, ("s_third", order), ("c_sum", order, 0))
        put(last, 5, ("z_sum", 1, 0))
        for order in range(2, last):
            put(last, 7, ("s_second", order))
    after = [("s_third", last), ("c_sum", last, 0)]
    after += [("c_sum", last, hop) for hop in range(1, 2 if last > 1 else 1)]
    after += [("c_sum", reach, hop) for reach in range(2, last) for hop in range(1, reach)]
    after += [("z_sum", reach, 0) for reach in range(2, last)]
    after += [("s_second", last), ("s_third", 0)]
    after += [("z_sum", last, 0)]
    after += [("z_sum", last, hop) for hop in range(1, 2 if last > 1 else 1)]
    after += [("c_sum", last, hop) for hop in range(2, last)]
    after += [("z_sum", reach, hop) for reach in range(2, last) for hop in range(1, reach)]
    after += [("s_second", 0)]
    after += [("c_back",)]
    after += [("z_sum", last, hop) for hop in range(2, last)]
    after += [("c_cross",), ("z_final",), ("c_final",)]
    return before, plan, after


def fused_body(tokens, gate_weights, expert_ids, w_gate, w_up, w_down):
    columns = lax.axis_size("grp")
    rows, width = tokens.shape
    experts, _, units = w_gate.shape
    deep = columns // 4
    half = rows // 2
    split = max(1, round(width * 2 / 9 / TILE)) * TILE
    edges = list(range(0, width, 4 * TILE)) + [width]
    tiles = list(zip(edges[:-1], edges[1:]))
    padded = -(-columns * experts // LANES) * LANES
    blocks = units // TILE
    bf16 = tokens.dtype
    dma = pltpu.SemaphoreType.DMA
    vmem = lambda *shape: pltpu.VMEM(shape, bf16)
    anywhere = pl.BlockSpec(memory_space=pl.ANY)
    local = pl.BlockSpec(memory_space=pltpu.VMEM)
    lined = columns * rows
    groups = 2 * (deep - 1) + 3 * deep + 5 + 2 * (deep - 1) + 2 * (deep - 2) + 3 * deep + 2 * deep * (deep - 1) + 2
    return pl.pallas_call(
        functools.partial(layer_kernel, columns, split, tiles),
        out_shape=jax.ShapeDtypeStruct((rows, width), bf16),
        in_specs=[anywhere, local, local, anywhere, anywhere, anywhere],
        out_specs=local,
        scratch_shapes=[
            vmem(2 * lined, width + padded),
            vmem(experts * blocks, width, TILE), vmem(experts * blocks, width, TILE),
            vmem(experts * units, width),
            vmem(8 * rows, experts * units),
            vmem(2 * lined, width), vmem(lined, width),
            vmem(deep * 4 * half, width), vmem(deep * rows, width),
            vmem(lined, width), vmem(lined, width),
            vmem(4 * rows, width),
            dma, dma((2,)), dma((experts,)), dma((groups,)), dma((2, columns)), dma((columns,)), dma((2,)),
            dma((deep,)), dma((deep,)), dma((deep, 2, 2)), dma((deep, 2)), dma((deep, 2)), dma((deep, 2)),
            dma((2,)), dma((2, 2)), dma((2,)), dma((columns,)), dma((columns,)), dma((4,)),
        ],
        compiler_params=pltpu.CompilerParams(
            collective_id=1, has_side_effects=True, vmem_limit_bytes=60 * 2**20),
        name="expert_layer",
    )(tokens, expert_ids.T, gate_weights.T, w_gate, w_up, w_down)


def expert_rows(inputs, scales, gate_part, up_part, down_part):
    gate_act = jnp.dot(inputs, gate_part, preferred_element_type=jnp.float32)
    upward = jnp.dot(inputs, up_part, preferred_element_type=jnp.float32)
    hidden = (jax.nn.silu(gate_act) * upward).astype(jnp.bfloat16)
    projected = lax.dot_general(
        hidden, down_part, (((1,), (1,)), ((), ())), preferred_element_type=jnp.float32
    )
    return projected * scales.astype(jnp.float32)[:, None]


def weights_path(rows_in, scales_in, w_gate, w_up, w_down):
    row_dims = rows_in.shape
    shard_units = w_gate.shape[2]
    expert_inputs = [rows_in[:, expert].reshape(-1, row_dims[3]) for expert in range(row_dims[1])]
    expert_scales = [scales_in[:, expert].reshape(-1) for expert in range(row_dims[1])]
    starting = tuple(
        (
            jnp.zeros((row_dims[0] * row_dims[2], row_dims[3]), jnp.float32)
            for expert in range(row_dims[1])
        )
    )
    gate_piece = lax.all_gather(w_gate, "loc", axis=2, tiled=True)
    up_piece = lax.all_gather(w_up, "loc", axis=2, tiled=True)
    down_piece = lax.all_gather(w_down, "loc", axis=2, tiled=True)
    updated = []
    for expert in range(row_dims[1]):
        running = starting[expert]
        for block_index in range(gate_piece.shape[2] // shard_units):
            lower_unit = block_index * shard_units
            upper_unit = lower_unit + shard_units
            values = expert_rows(
                expert_inputs[expert],
                expert_scales[expert],
                gate_piece[expert][:, lower_unit:upper_unit],
                up_piece[expert][:, lower_unit:upper_unit],
                down_piece[expert][:, lower_unit:upper_unit],
            )
            rounded = lax.optimization_barrier(values.astype(jnp.bfloat16))
            running = running + rounded.astype(jnp.float32)
        updated.append(running)
    folded = tuple(updated)
    stacked = jnp.stack(
        [folded_part.reshape(row_dims[0], row_dims[2], row_dims[3]) for folded_part in folded],
        axis=1,
    )
    return stacked.astype(jnp.bfloat16)


def slot_body(tokens, gate_weights, expert_ids, w_gate, w_up, w_down):
    tok_count = tokens.shape[0]
    choices_per = expert_ids.shape[1]
    feature_count = tokens.shape[1]
    group_count = lax.axis_size("grp")
    local_experts = w_gate.shape[0]
    expert_total = group_count * local_experts
    slot_depth = 2 * tok_count * RGROUPS // expert_total
    slot_total = expert_total * slot_depth
    pair_ids = expert_ids.reshape(-1)
    pair_count = pair_ids.shape[0]
    pair_order = jnp.arange(pair_count, dtype=jnp.int32)
    same_expert = (pair_ids[:, None] == pair_ids[None, :]).astype(jnp.int32)
    earlier = (pair_order[:, None] > pair_order[None, :]).astype(jnp.int32)
    slot_rank = jnp.sum(same_expert * earlier, axis=1)
    position = pair_ids * slot_depth + slot_rank
    pair_onehot = jnp.arange(slot_total, dtype=jnp.int32)[:, None] == position[None, :]
    placement = jnp.sum(
        pair_onehot.reshape(slot_total, tok_count, choices_per).astype(jnp.int32), axis=2
    ).astype(jnp.bfloat16)
    send_rows = jnp.dot(placement, tokens, preferred_element_type=jnp.float32).astype(jnp.bfloat16)
    flat_scales = gate_weights.reshape(-1).astype(jnp.float32)
    send_scales = jnp.sum(jnp.where(pair_onehot, flat_scales[None, :], 0.0), axis=1).astype(
        jnp.bfloat16
    )
    send_rows = send_rows.reshape(group_count, local_experts, slot_depth, feature_count)
    send_scales = send_scales.reshape(group_count, local_experts, slot_depth)
    computed = weights_path(
        lax.all_to_all(send_rows, "grp", split_axis=0, concat_axis=0, tiled=True),
        lax.all_to_all(send_scales, "grp", split_axis=0, concat_axis=0, tiled=True),
        w_gate,
        w_up,
        w_down,
    )
    returned = lax.all_to_all(computed, "grp", split_axis=0, concat_axis=0, tiled=True)
    flat_back = returned.reshape(slot_total, feature_count)
    mixed_out = lax.dot_general(
        placement, flat_back, (((0,), (0,)), ((), ())), preferred_element_type=jnp.float32
    )
    return mixed_out.astype(jnp.bfloat16)


def body(tokens, gate_weights, expert_ids, w_gate, w_up, w_down):
    tok_count, width = tokens.shape
    units = w_gate.shape[2]
    columns = lax.axis_size("grp")
    slot_depth = 2 * tok_count * RGROUPS // (columns * w_gate.shape[0])
    dense = slot_depth * w_gate.shape[0] >= tok_count
    fits = (columns % 4 == 0 and lax.axis_size("loc") == 2 and tok_count % 32 == 0
            and columns >= 8 and width % TILE == 0 and width > TILE
            and units % TILE == 0 and width % units == 0)
    chosen = fused_body if dense and fits else slot_body
    return chosen(tokens, gate_weights, expert_ids, w_gate, w_up, w_down)


def solution(mesh):
    placed = (
        P(("grp", "loc"), None),
        P(("grp", "loc"), None),
        P(("grp", "loc"), None),
        P("grp", None, "loc"),
        P("grp", None, "loc"),
        P("grp", None, "loc"),
    )
    return jax.shard_map(
        body, mesh=mesh, in_specs=placed, out_specs=P(("grp", "loc"), None), check_vma=False
    )
```

```python
import functools

import jax
import jax.numpy as jnp
from jax import lax
from jax.experimental import pallas as pl
from jax.experimental.pallas import tpu as pltpu
from jax.sharding import PartitionSpec as P

RGROUPS = 8
LANES = 128
TILE = 256
MESH = pl.DeviceIdType.MESH
FLIPS = ((1, 0), (0, 1))
HERE, DIAG = (0, 0), (1, 1)


class Place:
    def __init__(self, columns):
        self.deep = columns // 4
        self.g = lax.axis_index("grp")
        self.c = lax.axis_index("loc")
        self.x = lax.rem(self.g, 2)
        self.y = lax.rem(lax.div(self.g, 2), 2)
        self.z = lax.div(self.g, 4)
        self.below = self.z > 0
        self.above = self.z < self.deep - 1
        self.end = jnp.logical_or(self.z == 0, self.z == self.deep - 1)

    def spot(self, flip):
        x = 1 - self.x if flip[0] else self.x
        y = 1 - self.y if flip[1] else self.y
        return y * 2 + x

    def at(self, dz=0, flip=HERE):
        return (self.z + dz) * 4 + self.spot(flip)

    def line(self, step):
        if step == 0:
            return [(0, None)]
        return [(-step, self.z >= step), (step, self.z + step < self.deep)]

    def layer(self, order):
        picked = self.z
        for z in range(self.deep):
            ranked = sorted(range(self.deep), key=lambda other: (abs(other - z), other))
            picked = jnp.where(self.z == z, ranked[order], picked)
        return picked


def when(cond, act):
    if cond is None:
        act()
    else:
        pl.when(cond)(act)


def both(a, b):
    return b if a is None else jnp.logical_and(a, b)


def greet(me):
    barrier = pltpu.get_barrier_semaphore()
    partners = [
        (None, me.at(0, (1, 0)), me.c),
        (None, me.at(0, (0, 1)), me.c),
        (None, me.g, 1 - me.c),
        (me.below, me.at(-1), me.c),
        (me.above, me.at(1), me.c),
    ]
    for cond, g, c in partners:
        when(cond, lambda g=g, c=c: pl.semaphore_signal(
            barrier, inc=1, device_id=(g, c), device_id_type=MESH))
    edges = (me.z > 0).astype(jnp.int32) + (me.z < me.deep - 1).astype(jnp.int32)
    pl.semaphore_wait(barrier, 3 + edges)


def layer_kernel(columns, split, split_back, depth, tiles, tokens_hbm, ids_ref, gains_ref, wg_hbm, wu_hbm, wd_hbm, out_ref,
                 rows_ref, wg, wu, wd, place, weigh, packed, hid, back, part, mine, two, one, low, high,
                 far, own_sem, weight_sem, down_sem, send_sem, gz_ici, gc_ici, gc_half, core_sem,
                 sum_sem, two_sem, one_sem, low_sem, high_sem, far_sem,
                 xtwo_sem, xone_sem, clow_sem, chigh_sem):
    me = Place(columns)
    deep = me.deep
    rows, width = tokens_hbm.shape
    half = rows // 2
    lot = 8 * rows
    experts, _, units = wd_hbm.shape
    blocks = units // TILE
    lines = [me.line(step) for step in range(deep)]
    layers = [me.layer(order) for order in range(deep)]
    at_layer = [me.z == layer for layer in range(deep)]
    direct = slice(0, split)
    front, rest = slice(0, split_back), slice(split_back, width)
    carried = slice(split, rows_ref.shape[1])
    spots = (HERE,) + FLIPS + (DIAG,)
    sends = {}
    last = deep - 1
    jump = deep > 2

    own_rows = pl.multiple_of((me.z * 8 + me.c * 4 + me.spot(HERE)) * rows, rows)
    own_copy = pltpu.make_async_copy(
        tokens_hbm, rows_ref.at[pl.ds(own_rows, rows), 0:width], own_sem)
    own_copy.start()

    def weights():
        for e in range(experts):
            for b in range(width // units):
                pltpu.make_async_copy(
                    wd_hbm.at[e, b * units:(b + 1) * units, :],
                    wd.at[e * units:(e + 1) * units, b * units:(b + 1) * units], down_sem.at[e]).start()
        for s in range(experts * blocks):
            e, n = divmod(s, blocks)
            for kind, (source, target) in enumerate(((wg_hbm, wg), (wu_hbm, wu))):
                pltpu.make_async_copy(
                    source.at[e, :, n * TILE:(n + 1) * TILE], target.at[s], weight_sem.at[kind]).start()

    numbers = lax.broadcasted_iota(jnp.int32, (rows_ref.shape[1] - width, rows), 0)
    table = jnp.zeros(numbers.shape, jnp.float32)
    gains = gains_ref[...].astype(jnp.float32)
    ids = ids_ref[...]
    for k in range(ids.shape[0]):
        table = table + jnp.where(ids[k:k + 1, :] == numbers, gains[k:k + 1, :], 0.0)
    table = table.astype(rows_ref.dtype)
    unit = (lax.broadcasted_iota(jnp.int32, (rows, rows), 0)
            == lax.broadcasted_iota(jnp.int32, (rows, rows), 1)).astype(rows_ref.dtype)
    rows_ref[pl.ds(own_rows, rows), width:] = lax.dot_general(
        unit, table, (((1,), (1,)), ((), ())), preferred_element_type=jnp.float32).astype(rows_ref.dtype)
    greet(me)

    def row(c, layer, flip=HERE, h=0):
        return pl.multiple_of((layer * 8 + c * 4 + me.spot(flip)) * rows + h * half, half)

    def post(layer, flip=HERE, h=0):
        return pl.multiple_of((layer * 4 + me.spot(flip)) * rows + h * half, half)

    def column(layer, flip=HERE):
        return layer * 4 + me.spot(flip)

    def device(kind, h=0):
        return {
            "up": lambda: (me.at(1), me.c),
            "down": lambda: (me.at(-1), me.c),
            "near": lambda: (me.at(0, FLIPS[h]), me.c),
            "side": lambda: (me.at(0, FLIPS[1 - h]), me.c),
            "core": lambda: (me.g, 1 - me.c),
        }[kind]()

    def remote(source, target, send_sem, recv_sem, where):
        return pltpu.make_async_remote_copy(
            src_ref=source, dst_ref=target, send_sem=send_sem, recv_sem=recv_sem,
            device_id=where, device_id_type=MESH)

    def issue(key, cond, size, cols, make):
        number, _, total, _ = sends.get(key, (len(sends), cond, 0, cols))
        sends[key] = (number, cond, total + size, cols)
        when(cond(), lambda: make(send_sem.at[number]).start())

    def landed(ref, sem):
        remote(ref, ref, own_sem, sem, (me.g, 1 - me.c)).wait_recv()

    def always():
        return None

    def z_slot(h, layer, flip):
        return rows_ref.at[pl.ds(row(me.c, layer, flip, h), half), carried]

    def push_z(key, cond, h, layer, flip, kind):
        def make(sem):
            slot = z_slot(h, layer(), flip)
            recv = core_sem.at[layer()] if kind == "core" else gz_ici.at[h, column(layer(), flip)]
            return remote(slot, slot, sem, recv, device(kind, h))
        issue(key, cond, half, carried, make)

    def z_landed(h, layer, flip):
        landed(z_slot(h, layer, flip), gz_ici.at[h, column(layer, flip)])

    def c_slot(layer, flip, h=None):
        size = rows if h is None else half
        return rows_ref.at[pl.ds(row(me.c, layer, flip, h or 0), size), direct]

    def push_c(key, cond, layer, flip, kind, h=None, k=0):
        size = rows if h is None else half

        def make(sem):
            slot = c_slot(layer(), flip, h)
            recv = (core_sem.at[layer()] if kind == "core"
                    else gc_ici.at[column(layer(), flip)] if h is None else gc_half.at[h])
            return remote(slot, slot, sem, recv, device(kind, k))
        issue(key, cond, size, direct, make)

    def z_first(step):
        for dz, cond in lines[step]:
            layer = lambda dz=dz: me.z + dz
            for h in range(2):
                if step:
                    when(cond, lambda: z_landed(h, layer(), HERE))
                if dz <= 0 and step < last:
                    push_z(("up", dz), lambda cond=cond: both(cond, me.above), h, layer, HERE, "up")
                if dz >= 0 and step < last:
                    push_z(("down", dz), lambda cond=cond: both(cond, me.below), h, layer, HERE, "down")

    def z_cross(order):
        for kind in ("near", "side", "core"):
            for h in range(2):
                push_z("z", always, h, lambda: layers[order], HERE, kind)

    def z_second(order):
        for h in range(2):
            z_landed(h, layers[order], FLIPS[h])
            push_z("z", always, h, lambda: layers[order], FLIPS[h], "side")
            push_z("z", always, h, lambda: layers[order], FLIPS[h], "core")

    def z_third(order):
        for flips in (lambda h: FLIPS[1 - h], lambda h: DIAG):
            for h in range(2):
                z_landed(h, layers[order], flips(h))
                push_z("z", always, h, lambda: layers[order], flips(h), "core")

    def own():
        return me.z

    def along(flip):
        push_c("c up", lambda: me.above, own, flip, "up")
        push_c("c down", lambda: me.below, own, flip, "down")
        push_c("c", always, own, flip, "core")

    def c_first():
        for k in range(2):
            push_c("c", always, own, HERE, "near" if k == 0 else "side")
        along(HERE)

    def c_second():
        for k in range(2):
            landed(c_slot(me.z, FLIPS[k]), gc_ici.at[me.at(0, FLIPS[k])])
            push_c("c", always, own, FLIPS[k], "side", h=k, k=k)
            along(FLIPS[k])

    def c_third():
        for h in range(2):
            landed(c_slot(me.z, DIAG, h), gc_half.at[h])
        along(DIAG)

    def c_line(step):
        for dz, cond in lines[step]:
            layer = lambda dz=dz: me.z + dz
            for flip in spots:
                when(cond, lambda: landed(c_slot(layer(), flip), gc_ici.at[column(layer(), flip)]))
                if step < last:
                    edge, kind = (me.above, "up") if dz < 0 else (me.below, "down")
                    push_c(("c on", dz), lambda cond=cond, edge=edge: both(cond, edge), layer, flip, kind)
                push_c(("c in", dz), lambda cond=cond: cond, layer, flip, "core")

    def other_core(order):
        base = pl.multiple_of((layers[order] * 8 + (1 - me.c) * 4) * rows, 4 * rows)
        landed(rows_ref.at[pl.ds(base, 4 * rows), :], core_sem.at[layers[order]])

    def turn_down(e):
        whole = wd.at[e * units:(e + 1) * units, :]
        pltpu.make_async_copy(whole, whole, down_sem.at[e]).wait()
        for b in range(width // units):
            block = (slice(e * units, (e + 1) * units), slice(b * units, (b + 1) * units))
            wd[block] = wd[block].T

    share = 8 * depth

    def pack(order):
        base = pl.multiple_of(layers[order] * lot, lot)
        table = rows_ref[pl.ds(base, lot), width:].astype(jnp.float32)
        token = lax.broadcasted_iota(jnp.int32, (lot, lot), 0)
        other = lax.broadcasted_iota(jnp.int32, (lot, lot), 1)
        earlier = jnp.logical_and(other < token, lax.div(other, rows) == lax.div(token, rows))
        rank = jnp.dot(
            jnp.where(earlier, 1.0, 0.0).astype(place.dtype),
            jnp.where(table > 0.0, 1.0, 0.0).astype(place.dtype), preferred_element_type=jnp.float32)
        lane = lax.broadcasted_iota(jnp.int32, table.shape, 1)
        slot = lax.broadcasted_iota(jnp.int32, (lot, share), 1)
        first = lax.div(lax.broadcasted_iota(jnp.int32, (lot, share), 0), rows) * depth
        for e in range(experts):
            pick = lane == me.g * experts + e
            scale = jnp.sum(jnp.where(pick, table, 0.0), axis=1, keepdims=True)
            mine_rank = jnp.sum(jnp.where(pick, rank, 0.0), axis=1, keepdims=True)
            hit = jnp.logical_and((slot - first).astype(jnp.float32) == mine_rank, scale > 0.0)
            place[:, e * share:(e + 1) * share] = jnp.where(hit, 1.0, 0.0).astype(place.dtype)
            weigh[:, e * share:(e + 1) * share] = jnp.where(hit, scale, 0.0).astype(weigh.dtype)
        for cols in tiles:
            cols = slice(*cols)
            packed[:, cols] = lax.dot_general(
                place[...], rows_ref[pl.ds(base, lot), cols], (((0,), (0,)), ((), ())),
                preferred_element_type=jnp.float32).astype(packed.dtype)

    def hidden_step(order, s):
        del order
        e, n = lax.div(s, blocks), lax.rem(s, blocks)
        start = pl.multiple_of(e * share, share)
        x = packed[pl.ds(start, share), :]
        gate = jnp.dot(x, wg[s], preferred_element_type=jnp.float32)
        upward = jnp.dot(x, wu[s], preferred_element_type=jnp.float32)
        value = jax.nn.silu(gate) * upward
        hid[pl.ds(start, share), pl.ds(pl.multiple_of(n * TILE, TILE), TILE)] = value.astype(hid.dtype)

    def down_step(order, t):
        base = pl.multiple_of(layers[order] * lot, lot)
        cols = slice(*tiles[t])
        span = slice(0, tiles[t][1] - tiles[t][0])
        for e in range(experts):
            mix = slice(e * share, (e + 1) * share)
            back[mix, span] = jnp.dot(
                hid[mix, :], wd[e * units:(e + 1) * units, cols],
                preferred_element_type=jnp.float32).astype(back.dtype)
        part[pl.ds(base, lot), cols] = jnp.dot(
            weigh[...], back[:, span], preferred_element_type=jnp.float32).astype(part.dtype)

        def make(sem):
            start = pl.multiple_of((layers[order] * 8 + (1 - me.c) * 4) * rows, 4 * rows)
            there = pl.multiple_of(layers[order] * 4 * rows, 4 * rows)
            return remote(
                part.at[pl.ds(start, 4 * rows), cols], mine.at[pl.ds(there, 4 * rows), cols],
                sem, sum_sem.at[layers[order]], device("core"))
        tail = slice(0, width) if t == len(tiles) - 1 else cols
        issue("part", always, 4 * rows if t == len(tiles) - 1 else 0, tail, make)

    def add(size, cols, terms, target, start):
        for at in range(cols.start, cols.stop, TILE):
            piece = slice(at, at + TILE)
            total = None
            for ref, base in terms:
                term = ref[pl.ds(base, size), piece].astype(jnp.float32)
                total = term if total is None else total + term
            target[pl.ds(start, size), piece] = total.astype(target.dtype)

    def own_terms(layer, flip, h=0):
        return [(part, row(me.c, layer, flip, h)), (mine, post(layer, flip, h))]

    def from_core(order):
        start = pl.multiple_of(layers[order] * 4 * rows, 4 * rows)
        landed(mine.at[pl.ds(start, 4 * rows), :], sum_sem.at[layers[order]])

    def two_at(layer, j, h):
        return pl.multiple_of(((layer * 2 + j) * 2 + h) * half, half)

    def one_at(layer, h):
        return pl.multiple_of((layer * 2 + h) * half, half)

    def two_slot(layer, j, h, cols):
        return two.at[pl.ds(two_at(layer, j, h), half), cols]

    def one_slot(layer, h, cols):
        return one.at[pl.ds(one_at(layer, h), half), cols]

    def send_sum(key, cond, layer, flip, h, size, cols, target, recv_sem, where):
        def make(sem):
            return remote(
                mine.at[pl.ds(post(layer(), flip, h), size), cols], target(), sem, recv_sem(), where())
        issue(key, cond, size, cols, make)

    def s_third(order, only=None):
        layer = lambda: layers[order]
        if only != 0:
            from_core(order)
        for j, flips in ((1, lambda h: DIAG), (0, lambda h: FLIPS[1 - h])):
            if only not in (None, j):
                continue
            for h in range(2):
                flip = flips(h)
                add(half, rest, own_terms(layer(), flip, h), mine, post(layer(), flip, h))
                send_sum(
                    "s", always, layer, flip, h, half, rest,
                    lambda j=j, h=h: two_slot(layer(), j, h, rest),
                    lambda j=j, h=h: two_sem.at[layer(), j, h], lambda h=h: device("side", h))

    def s_second(order):
        layer = lambda: layers[order]
        for h in range(2):
            flip = FLIPS[h]
            landed(two_slot(layer(), 1, h, rest), two_sem.at[layer(), 1, h])
            add(half, rest, own_terms(layer(), flip, h) + [(two, two_at(layer(), 1, h))],
                mine, post(layer(), flip, h))
            send_sum(
                "s", always, layer, flip, h, half, rest,
                lambda h=h: one_slot(layer(), h, rest), lambda h=h: one_sem.at[layer(), h],
                lambda h=h: device("near", h))

    def columns_in(layer, h):
        landed(two_slot(layer, 0, h, rest), two_sem.at[layer, 0, h])
        landed(one_slot(layer, h, rest), one_sem.at[layer, h])
        return own_terms(layer, HERE, h) + [(two, two_at(layer, 0, h)), (one, one_at(layer, h))]

    def ways(reach, hop, leap):
        for cond, to, name in (
                (at_layer[hop], reach, "up"), (at_layer[deep - 1 - hop], deep - 1 - reach, "down")):
            over = leap and reach == last and hop == 0
            joins = hop > (1 if leap and reach == last else 0)
            near, z_sem, c_sem = (low, low_sem, clow_sem) if name == "up" else (high, high_sem, chigh_sem)
            yield cond, to, name, over, joins, near, z_sem, c_sem

    def z_sum(reach, hop, only=None):
        for h in (0, 1) if only is None else (only,):
            for cond, to, name, over, joins, near, sem, _ in ways(reach, hop, jump and h == 0):
                def act():
                    terms = columns_in(to, h)
                    if joins:
                        landed(near.at[pl.ds(post(to, HERE, h), half), rest], sem.at[to, h])
                        terms.append((near, post(to, HERE, h)))
                    add(half, rest, terms, mine, post(to, HERE, h))
                pl.when(cond)(act)

                def target(to=to, near=near, over=over, h=h):
                    ref, at = (far, post(0, HERE, h)) if over else (near, post(to, HERE, h))
                    return ref.at[pl.ds(at, half), rest]
                send_sum(
                    ("z sum", name, hop), lambda cond=cond: cond, lambda to=to: to, HERE, h, half,
                    rest, target,
                    lambda to=to, sem=sem, over=over, h=h: far_sem.at[h] if over else sem.at[to, h],
                    lambda to=to, name=name, over=over: (
                        (column(to), me.c) if over else device(name)))

    def c_sum(reach, hop):
        for cond, to, name, _, joins, near, _, sem in ways(reach, hop, False):
            for flip in spots:
                def act():
                    terms = own_terms(to, flip)
                    if joins:
                        landed(near.at[pl.ds(post(to, flip), rows), front], sem.at[column(to, flip)])
                        terms.append((near, post(to, flip)))
                    add(rows, front, terms, mine, post(to, flip))
                pl.when(cond)(act)
                send_sum(
                    ("c sum", name, hop), lambda cond=cond: cond, lambda to=to: to, flip, 0, rows, front,
                    lambda to=to, near=near, flip=flip: near.at[pl.ds(post(to, flip), rows), front],
                    lambda to=to, sem=sem, flip=flip: sem.at[column(to, flip)],
                    lambda name=name: device(name))

    def lined(flip, h, leap):
        beyond = [(low, post(me.z, flip, h)), (high, post(me.z, flip, h))]
        return own_terms(me.z, flip, h) + beyond + ([(far, post(0, flip, h))] if leap else [])

    def z_final():
        for h in range(2):
            terms = columns_in(me.z, h)[2:] + lined(HERE, h, jump and h == 0)
            spot = pl.ds(post(me.z, HERE, h), half)
            pl.when(me.below)(lambda: landed(low.at[spot, rest], low_sem.at[me.z, h]))
            pl.when(me.above)(lambda: landed(high.at[spot, rest], high_sem.at[me.z, h]))
            if jump and h == 0:
                spot_far = pl.ds(post(0, HERE, h), half)
                pl.when(me.end)(lambda: landed(far.at[spot_far, rest], far_sem.at[h]))
            add(half, rest, terms, out_ref, h * half)

    def c_back():
        for flip in (DIAG,) + FLIPS + (HERE,):
            g = column(me.z, flip)
            spot = pl.ds(post(me.z, flip), rows)
            pl.when(me.below)(lambda: landed(low.at[spot, front], clow_sem.at[g]))
            pl.when(me.above)(lambda: landed(high.at[spot, front], chigh_sem.at[g]))
        for j, flips in ((1, lambda h: DIAG), (0, lambda h: FLIPS[1 - h])):
            for h in range(2):
                flip = flips(h)
                add(half, front, lined(flip, h, False), mine, post(me.z, flip, h))
                send_sum(
                    "c sum", always, own, flip, h, half, front,
                    lambda j=j, h=h: two_slot(me.z, j, h, front),
                    lambda j=j, h=h: xtwo_sem.at[j, h], lambda h=h: device("side", h))

    def c_cross():
        for h in range(2):
            flip = FLIPS[h]
            landed(two_slot(me.z, 1, h, front), xtwo_sem.at[1, h])
            add(half, front, lined(flip, h, False) + [(two, two_at(me.z, 1, h))], mine, post(me.z, flip, h))
            send_sum(
                "c sum", always, own, flip, h, half, front, lambda h=h: one_slot(me.z, h, front),
                lambda h=h: xone_sem.at[h], lambda h=h: device("near", h))

    def c_final():
        for h in range(2):
            landed(two_slot(me.z, 0, h, front), xtwo_sem.at[0, h])
            landed(one_slot(me.z, h, front), xone_sem.at[h])
            add(half, front, lined(HERE, h, False) + [(two, two_at(me.z, 0, h)), (one, one_at(me.z, h))],
                out_ref, h * half)

    def clear(ref, layer):
        base = layer * 4 * rows

        def body(i, carry):
            ref[pl.ds(pl.multiple_of(base + i * half, half), half), :] = jnp.zeros((half, width), ref.dtype)
            return carry
        lax.fori_loop(0, 8, body, None)

    do = dict(
        z_first=z_first, z_cross=z_cross, z_second=z_second, z_third=z_third, c_first=c_first, c_second=c_second,
        c_third=c_third, c_line=c_line, turn_down=turn_down, s_third=s_third, s_second=s_second,
        z_sum=z_sum, c_sum=c_sum, z_final=z_final, c_back=c_back, c_cross=c_cross, c_final=c_final,
        weights=weights,
        clear_low=lambda: pl.when(jnp.logical_not(me.below))(lambda: clear(low, me.z)),
        clear_high=lambda: pl.when(jnp.logical_not(me.above))(lambda: clear(high, me.z)),
        clear_far=lambda: pl.when(jnp.logical_not(me.end))(lambda: clear(far, 0)))
    before, plan, after = order_of_work(deep, experts)

    def run(acts):
        for name, *args in acts:
            do[name](*args)

    own_copy.wait()
    run(before)
    for kind, ref in enumerate((wg, wu)):
        pltpu.make_async_copy(ref, ref, weight_sem.at[kind]).wait()
    subs = experts * blocks
    for order in range(deep):
        other_core(order)
        acts = plan[order]
        pack(order)

        def body(s, carry, order=order, acts=acts):
            for k in range(subs):
                if acts.get(k):
                    pl.when(s == k)(lambda k=k: run(acts[k]))
            hidden_step(order, s)
            return carry
        lax.fori_loop(0, subs, body, None)
        for t in range(len(tiles)):
            run(acts.get(subs + t, []))
            down_step(order, t)
    run(after)
    assert len(sends) == send_sem.shape[0], len(sends)
    for number, cond, total, cols in sends.values():
        spent = rows_ref.at[pl.ds(0, total), cols]
        when(cond(), lambda: remote(
            spent, spent, send_sem.at[number], own_sem, (me.g, 1 - me.c)).wait_send())


def order_of_work(deep, experts):
    last = deep - 1
    before = [("c_first",), ("z_first", 0), ("z_cross", 0), ("weights",)]
    before += [("clear_low",), ("clear_high",), ("clear_far",)]
    before += [("c_second",), ("turn_down", 0)]
    before += [("z_second", 0), ("z_first", 1), ("z_cross", 1)]
    before += [("turn_down", e) for e in range(1, experts)]
    before += [("c_third",), ("z_third", 0)]
    plan = [{} for _ in range(deep)]

    def put(order, step, *acts):
        plan[min(order, last)].setdefault(step, []).extend(acts)

    put(0, 1, ("z_second", 1))
    for order in range(last):
        if order:
            put(order - 1, 7, ("z_second", order + 1))
        if order + 2 < deep:
            put(order, 0 if order else 2, ("z_first", order + 2), ("z_cross", order + 2))
        put(order, (2, 5, 4)[order] if deep == 4 else 2, ("c_line", order + 1))
        put(order, (6, 5, 5)[order] if deep == 4 else 5, ("z_third", order + 1))
    if last > 1:
        put(last - 1, 1, ("s_third", 1), ("c_sum", 1, 0))
        put(last - 1, 3, ("s_third", 0, 1))
        put(last, 7, ("z_sum", 1, 0))
        put(last, 0, ("s_second", 1))
        for order in range(2, last):
            put(last, 0, ("s_third", order), ("c_sum", order, 0))
    else:
        put(last, 0, ("s_third", 0))
    after = [("s_second", order) for order in range(2, last)]
    after += [("s_third", last), ("c_sum", last, 0)]
    after += [("c_sum", reach, hop) for reach in range(2, last) for hop in range(1, reach)]
    after += [("s_second", last)]
    if last > 1:
        after += [("s_third", 0, 0)]
    after += [("z_sum", reach, 0) for reach in range(2, last)]
    after += [("c_sum", last, hop) for hop in range(1, 2 if last > 1 else 1)]
    after += [("z_sum", last, 0, 1), ("z_sum", last, 0, 0)]
    after += [("z_sum", last, hop, 0) for hop in range(1, 2 if last > 1 else 1)]
    after += [("c_sum", last, hop) for hop in range(2, last)]
    after += [("z_sum", last, hop, 1) for hop in range(1, 2 if last > 1 else 1)]
    after += [("z_sum", reach, hop) for reach in range(2, last) for hop in range(1, reach)]
    after += [("s_second", 0), ("c_back",)]
    after += [("z_sum", last, hop, h) for hop in range(2, last) for h in range(2)]
    after += [("c_cross",), ("z_final",), ("c_final",)]
    return before, plan, after


def fused_body(tokens, gate_weights, expert_ids, w_gate, w_up, w_down):
    columns = lax.axis_size("grp")
    rows, width = tokens.shape
    experts, _, units = w_gate.shape
    deep = columns // 4
    half = rows // 2
    split = max(1, round(width * 2 / 9 / TILE)) * TILE
    split_back = max(1, round(width / 7 / TILE)) * TILE
    edges = list(range(0, width, 4 * TILE)) + [width]
    tiles = list(zip(edges[:-1], edges[1:]))
    padded = -(-columns * experts // LANES) * LANES
    blocks = units // TILE
    bf16 = tokens.dtype
    depth = 2 * rows * RGROUPS // (columns * experts)
    dma = pltpu.SemaphoreType.DMA
    vmem = lambda *shape: pltpu.VMEM(shape, bf16)
    anywhere = pl.BlockSpec(memory_space=pl.ANY)
    local = pl.BlockSpec(memory_space=pltpu.VMEM)
    lined = columns * rows
    groups = 8 * (deep - 1) + 2 * (deep - 2) + 7
    return pl.pallas_call(
        functools.partial(layer_kernel, columns, split, split_back, depth, tiles),
        out_shape=jax.ShapeDtypeStruct((rows, width), bf16),
        in_specs=[anywhere, local, local, anywhere, anywhere, anywhere],
        out_specs=local,
        scratch_shapes=[
            vmem(2 * lined, width + padded),
            vmem(experts * blocks, width, TILE), vmem(experts * blocks, width, TILE),
            vmem(experts * units, width),
            vmem(8 * rows, experts * 8 * depth), vmem(8 * rows, experts * 8 * depth),
            vmem(experts * 8 * depth, width), vmem(experts * 8 * depth, units),
            vmem(experts * 8 * depth, 4 * TILE),
            vmem(2 * lined, width), vmem(lined, width),
            vmem(deep * 4 * half, width), vmem(deep * rows, width),
            vmem(lined, width), vmem(lined, width),
            vmem(4 * rows, width),
            dma, dma((2,)), dma((experts,)), dma((groups,)), dma((2, columns)), dma((columns,)), dma((2,)),
            dma((deep,)), dma((deep,)), dma((deep, 2, 2)), dma((deep, 2)), dma((deep, 2)), dma((deep, 2)),
            dma((2,)), dma((2, 2)), dma((2,)), dma((columns,)), dma((columns,)),
        ],
        compiler_params=pltpu.CompilerParams(
            collective_id=1, has_side_effects=True, vmem_limit_bytes=54 * 2**20),
        name="expert_layer",
    )(tokens, expert_ids.T, gate_weights.T, w_gate, w_up, w_down)


def expert_rows(inputs, scales, gate_part, up_part, down_part):
    gate_act = jnp.dot(inputs, gate_part, preferred_element_type=jnp.float32)
    upward = jnp.dot(inputs, up_part, preferred_element_type=jnp.float32)
    hidden = (jax.nn.silu(gate_act) * upward).astype(jnp.bfloat16)
    projected = lax.dot_general(
        hidden, down_part, (((1,), (1,)), ((), ())), preferred_element_type=jnp.float32
    )
    return projected * scales.astype(jnp.float32)[:, None]


def weights_path(rows_in, scales_in, w_gate, w_up, w_down):
    row_dims = rows_in.shape
    shard_units = w_gate.shape[2]
    expert_inputs = [rows_in[:, expert].reshape(-1, row_dims[3]) for expert in range(row_dims[1])]
    expert_scales = [scales_in[:, expert].reshape(-1) for expert in range(row_dims[1])]
    starting = tuple(
        (
            jnp.zeros((row_dims[0] * row_dims[2], row_dims[3]), jnp.float32)
            for expert in range(row_dims[1])
        )
    )
    gate_piece = lax.all_gather(w_gate, "loc", axis=2, tiled=True)
    up_piece = lax.all_gather(w_up, "loc", axis=2, tiled=True)
    down_piece = lax.all_gather(w_down, "loc", axis=2, tiled=True)
    updated = []
    for expert in range(row_dims[1]):
        running = starting[expert]
        for block_index in range(gate_piece.shape[2] // shard_units):
            lower_unit = block_index * shard_units
            upper_unit = lower_unit + shard_units
            values = expert_rows(
                expert_inputs[expert],
                expert_scales[expert],
                gate_piece[expert][:, lower_unit:upper_unit],
                up_piece[expert][:, lower_unit:upper_unit],
                down_piece[expert][:, lower_unit:upper_unit],
            )
            rounded = lax.optimization_barrier(values.astype(jnp.bfloat16))
            running = running + rounded.astype(jnp.float32)
        updated.append(running)
    folded = tuple(updated)
    stacked = jnp.stack(
        [folded_part.reshape(row_dims[0], row_dims[2], row_dims[3]) for folded_part in folded],
        axis=1,
    )
    return stacked.astype(jnp.bfloat16)


def slot_body(tokens, gate_weights, expert_ids, w_gate, w_up, w_down):
    tok_count = tokens.shape[0]
    choices_per = expert_ids.shape[1]
    feature_count = tokens.shape[1]
    group_count = lax.axis_size("grp")
    local_experts = w_gate.shape[0]
    expert_total = group_count * local_experts
    slot_depth = 2 * tok_count * RGROUPS // expert_total
    slot_total = expert_total * slot_depth
    pair_ids = expert_ids.reshape(-1)
    pair_count = pair_ids.shape[0]
    pair_order = jnp.arange(pair_count, dtype=jnp.int32)
    same_expert = (pair_ids[:, None] == pair_ids[None, :]).astype(jnp.int32)
    earlier = (pair_order[:, None] > pair_order[None, :]).astype(jnp.int32)
    slot_rank = jnp.sum(same_expert * earlier, axis=1)
    position = pair_ids * slot_depth + slot_rank
    pair_onehot = jnp.arange(slot_total, dtype=jnp.int32)[:, None] == position[None, :]
    placement = jnp.sum(
        pair_onehot.reshape(slot_total, tok_count, choices_per).astype(jnp.int32), axis=2
    ).astype(jnp.bfloat16)
    send_rows = jnp.dot(placement, tokens, preferred_element_type=jnp.float32).astype(jnp.bfloat16)
    flat_scales = gate_weights.reshape(-1).astype(jnp.float32)
    send_scales = jnp.sum(jnp.where(pair_onehot, flat_scales[None, :], 0.0), axis=1).astype(
        jnp.bfloat16
    )
    send_rows = send_rows.reshape(group_count, local_experts, slot_depth, feature_count)
    send_scales = send_scales.reshape(group_count, local_experts, slot_depth)
    computed = weights_path(
        lax.all_to_all(send_rows, "grp", split_axis=0, concat_axis=0, tiled=True),
        lax.all_to_all(send_scales, "grp", split_axis=0, concat_axis=0, tiled=True),
        w_gate,
        w_up,
        w_down,
    )
    returned = lax.all_to_all(computed, "grp", split_axis=0, concat_axis=0, tiled=True)
    flat_back = returned.reshape(slot_total, feature_count)
    mixed_out = lax.dot_general(
        placement, flat_back, (((0,), (0,)), ((), ())), preferred_element_type=jnp.float32
    )
    return mixed_out.astype(jnp.bfloat16)


def body(tokens, gate_weights, expert_ids, w_gate, w_up, w_down):
    tok_count, width = tokens.shape
    units = w_gate.shape[2]
    columns = lax.axis_size("grp")
    slot_depth = 2 * tok_count * RGROUPS // (columns * w_gate.shape[0])
    dense = slot_depth * w_gate.shape[0] >= tok_count
    fits = (columns % 4 == 0 and lax.axis_size("loc") == 2 and tok_count % 32 == 0
            and columns >= 8 and width % TILE == 0 and width > TILE
            and units % TILE == 0 and width % units == 0 and 8 * slot_depth % LANES == 0)
    chosen = fused_body if dense and fits else slot_body
    return chosen(tokens, gate_weights, expert_ids, w_gate, w_up, w_down)


def solution(mesh):
    placed = (
        P(("grp", "loc"), None),
        P(("grp", "loc"), None),
        P(("grp", "loc"), None),
        P("grp", None, "loc"),
        P("grp", None, "loc"),
        P("grp", None, "loc"),
    )
    return jax.shard_map(
        body, mesh=mesh, in_specs=placed, out_specs=P(("grp", "loc"), None), check_vma=False
    )
```

```python
import functools

import jax
import jax.numpy as jnp
from jax import lax
from jax.experimental import pallas as pl
from jax.experimental.pallas import tpu as pltpu
from jax.sharding import PartitionSpec as P

RGROUPS = 8
LANES = 128
TILE = 256
MESH = pl.DeviceIdType.MESH
FLIPS = ((1, 0), (0, 1))
HERE, DIAG = (0, 0), (1, 1)


class Place:
    def __init__(self, columns):
        self.deep = columns // 4
        self.g = lax.axis_index("grp")
        self.c = lax.axis_index("loc")
        self.x = lax.rem(self.g, 2)
        self.y = lax.rem(lax.div(self.g, 2), 2)
        self.z = lax.div(self.g, 4)
        self.below = self.z > 0
        self.above = self.z < self.deep - 1
        self.end = jnp.logical_or(self.z == 0, self.z == self.deep - 1)

    def spot(self, flip):
        x = 1 - self.x if flip[0] else self.x
        y = 1 - self.y if flip[1] else self.y
        return y * 2 + x

    def at(self, dz=0, flip=HERE):
        return (self.z + dz) * 4 + self.spot(flip)

    def line(self, step):
        if step == 0:
            return [(0, None)]
        return [(-step, self.z >= step), (step, self.z + step < self.deep)]

    def layer(self, order):
        picked = self.z
        for z in range(self.deep):
            ranked = sorted(range(self.deep), key=lambda other: (abs(other - z), other))
            picked = jnp.where(self.z == z, ranked[order], picked)
        return picked


def when(cond, act):
    if cond is None:
        act()
    else:
        pl.when(cond)(act)


def both(a, b):
    return b if a is None else jnp.logical_and(a, b)


def greet(me):
    barrier = pltpu.get_barrier_semaphore()
    partners = [
        (None, me.at(0, (1, 0)), me.c),
        (None, me.at(0, (0, 1)), me.c),
        (None, me.g, 1 - me.c),
        (me.below, me.at(-1), me.c),
        (me.above, me.at(1), me.c),
    ]
    for cond, g, c in partners:
        when(cond, lambda g=g, c=c: pl.semaphore_signal(
            barrier, inc=1, device_id=(g, c), device_id_type=MESH))
    edges = (me.z > 0).astype(jnp.int32) + (me.z < me.deep - 1).astype(jnp.int32)
    pl.semaphore_wait(barrier, 3 + edges)


def layer_kernel(columns, split, split_back, depth, tiles, tokens_hbm, ids_ref, gains_ref, wg_hbm, wu_hbm, wd_hbm, out_ref,
                 rows_ref, wg, wu, wd, place, weigh, packed, hid, back, part, mine, two, one, low, high,
                 far, own_sem, weight_sem, down_sem, send_sem, gz_ici, gc_ici, gc_half, core_sem,
                 sum_sem, two_sem, one_sem, low_sem, high_sem, far_sem,
                 xtwo_sem, xone_sem, clow_sem, chigh_sem):
    me = Place(columns)
    deep = me.deep
    rows, width = tokens_hbm.shape
    half = rows // 2
    lot = 8 * rows
    experts, _, units = wd_hbm.shape
    blocks = units // TILE
    lines = [me.line(step) for step in range(deep)]
    layers = [me.layer(order) for order in range(deep)]
    at_layer = [me.z == layer for layer in range(deep)]
    direct = slice(0, split)
    front, rest = slice(0, split_back), slice(split_back, width)
    carried = slice(split, rows_ref.shape[1])
    spots = (HERE,) + FLIPS + (DIAG,)
    sends = {}
    last = deep - 1
    jump = deep > 2

    own_rows = pl.multiple_of((me.z * 8 + me.c * 4 + me.spot(HERE)) * rows, rows)
    own_copy = pltpu.make_async_copy(
        tokens_hbm, rows_ref.at[pl.ds(own_rows, rows), 0:width], own_sem)
    own_copy.start()

    def weights():
        for e in range(experts):
            for b in range(width // units):
                pltpu.make_async_copy(
                    wd_hbm.at[e, b * units:(b + 1) * units, :],
                    wd.at[e * units:(e + 1) * units, b * units:(b + 1) * units], down_sem.at[e]).start()
        for s in range(experts * blocks):
            e, n = divmod(s, blocks)
            for kind, (source, target) in enumerate(((wg_hbm, wg), (wu_hbm, wu))):
                pltpu.make_async_copy(
                    source.at[e, :, n * TILE:(n + 1) * TILE], target.at[s], weight_sem.at[kind]).start()

    numbers = lax.broadcasted_iota(jnp.int32, (rows_ref.shape[1] - width, rows), 0)
    table = jnp.zeros(numbers.shape, jnp.float32)
    gains = gains_ref[...].astype(jnp.float32)
    ids = ids_ref[...]
    for k in range(ids.shape[0]):
        table = table + jnp.where(ids[k:k + 1, :] == numbers, gains[k:k + 1, :], 0.0)
    table = table.astype(rows_ref.dtype)
    unit = (lax.broadcasted_iota(jnp.int32, (rows, rows), 0)
            == lax.broadcasted_iota(jnp.int32, (rows, rows), 1)).astype(rows_ref.dtype)
    rows_ref[pl.ds(own_rows, rows), width:] = lax.dot_general(
        unit, table, (((1,), (1,)), ((), ())), preferred_element_type=jnp.float32).astype(rows_ref.dtype)
    greet(me)

    def row(c, layer, flip=HERE, h=0):
        return pl.multiple_of((layer * 8 + c * 4 + me.spot(flip)) * rows + h * half, half)

    def post(layer, flip=HERE, h=0):
        return pl.multiple_of((layer * 4 + me.spot(flip)) * rows + h * half, half)

    def column(layer, flip=HERE):
        return layer * 4 + me.spot(flip)

    def device(kind, h=0):
        return {
            "up": lambda: (me.at(1), me.c),
            "down": lambda: (me.at(-1), me.c),
            "near": lambda: (me.at(0, FLIPS[h]), me.c),
            "side": lambda: (me.at(0, FLIPS[1 - h]), me.c),
            "core": lambda: (me.g, 1 - me.c),
        }[kind]()

    def remote(source, target, send_sem, recv_sem, where):
        return pltpu.make_async_remote_copy(
            src_ref=source, dst_ref=target, send_sem=send_sem, recv_sem=recv_sem,
            device_id=where, device_id_type=MESH)

    def issue(key, cond, size, cols, make):
        number, _, total, _ = sends.get(key, (len(sends), cond, 0, cols))
        sends[key] = (number, cond, total + size, cols)
        when(cond(), lambda: make(send_sem.at[number]).start())

    def landed(ref, sem):
        remote(ref, ref, own_sem, sem, (me.g, 1 - me.c)).wait_recv()

    def always():
        return None

    def z_slot(h, layer, flip):
        return rows_ref.at[pl.ds(row(me.c, layer, flip, h), half), carried]

    def push_z(key, cond, h, layer, flip, kind):
        def make(sem):
            slot = z_slot(h, layer(), flip)
            recv = core_sem.at[layer()] if kind == "core" else gz_ici.at[h, column(layer(), flip)]
            return remote(slot, slot, sem, recv, device(kind, h))
        issue(key, cond, half, carried, make)

    def z_landed(h, layer, flip):
        landed(z_slot(h, layer, flip), gz_ici.at[h, column(layer, flip)])

    def c_slot(layer, flip, h=None):
        size = rows if h is None else half
        return rows_ref.at[pl.ds(row(me.c, layer, flip, h or 0), size), direct]

    def push_c(key, cond, layer, flip, kind, h=None, k=0):
        size = rows if h is None else half

        def make(sem):
            slot = c_slot(layer(), flip, h)
            recv = (core_sem.at[layer()] if kind == "core"
                    else gc_ici.at[column(layer(), flip)] if h is None else gc_half.at[h])
            return remote(slot, slot, sem, recv, device(kind, k))
        issue(key, cond, size, direct, make)

    def z_first(step):
        for dz, cond in lines[step]:
            layer = lambda dz=dz: me.z + dz
            for h in range(2):
                if step:
                    when(cond, lambda: z_landed(h, layer(), HERE))
                if dz <= 0 and step < last:
                    push_z(("up", dz), lambda cond=cond: both(cond, me.above), h, layer, HERE, "up")
                if dz >= 0 and step < last:
                    push_z(("down", dz), lambda cond=cond: both(cond, me.below), h, layer, HERE, "down")

    def z_cross(order):
        for kind in ("near", "side", "core"):
            for h in range(2):
                push_z("z", always, h, lambda: layers[order], HERE, kind)

    def z_second(order):
        for h in range(2):
            z_landed(h, layers[order], FLIPS[h])
            push_z("z", always, h, lambda: layers[order], FLIPS[h], "side")
            push_z("z", always, h, lambda: layers[order], FLIPS[h], "core")

    def z_third(order):
        for flips in (lambda h: FLIPS[1 - h], lambda h: DIAG):
            for h in range(2):
                z_landed(h, layers[order], flips(h))
                push_z("z", always, h, lambda: layers[order], flips(h), "core")

    def own():
        return me.z

    def along(flip):
        push_c("c up", lambda: me.above, own, flip, "up")
        push_c("c down", lambda: me.below, own, flip, "down")
        push_c("c", always, own, flip, "core")

    def c_first():
        for k in range(2):
            push_c("c", always, own, HERE, "near" if k == 0 else "side")
        along(HERE)

    def c_second():
        for k in range(2):
            landed(c_slot(me.z, FLIPS[k]), gc_ici.at[me.at(0, FLIPS[k])])
            push_c("c", always, own, FLIPS[k], "side", h=k, k=k)
            along(FLIPS[k])

    def c_third():
        for h in range(2):
            landed(c_slot(me.z, DIAG, h), gc_half.at[h])
        along(DIAG)

    def c_line(step):
        for dz, cond in lines[step]:
            layer = lambda dz=dz: me.z + dz
            for flip in spots:
                when(cond, lambda: landed(c_slot(layer(), flip), gc_ici.at[column(layer(), flip)]))
                if step < last:
                    edge, kind = (me.above, "up") if dz < 0 else (me.below, "down")
                    push_c(("c on", dz), lambda cond=cond, edge=edge: both(cond, edge), layer, flip, kind)
                push_c(("c in", dz), lambda cond=cond: cond, layer, flip, "core")

    def other_core(order):
        base = pl.multiple_of((layers[order] * 8 + (1 - me.c) * 4) * rows, 4 * rows)
        landed(rows_ref.at[pl.ds(base, 4 * rows), :], core_sem.at[layers[order]])

    def turn_down(e):
        whole = wd.at[e * units:(e + 1) * units, :]
        pltpu.make_async_copy(whole, whole, down_sem.at[e]).wait()
        for b in range(width // units):
            block = (slice(e * units, (e + 1) * units), slice(b * units, (b + 1) * units))
            wd[block] = wd[block].T

    share = 8 * depth

    def pack(order):
        base = pl.multiple_of(layers[order] * lot, lot)
        table = rows_ref[pl.ds(base, lot), width:].astype(jnp.float32)
        token = lax.broadcasted_iota(jnp.int32, (lot, lot), 0)
        other = lax.broadcasted_iota(jnp.int32, (lot, lot), 1)
        earlier = jnp.logical_and(other < token, lax.div(other, rows) == lax.div(token, rows))
        rank = jnp.dot(
            jnp.where(earlier, 1.0, 0.0).astype(place.dtype),
            jnp.where(table > 0.0, 1.0, 0.0).astype(place.dtype), preferred_element_type=jnp.float32)
        lane = lax.broadcasted_iota(jnp.int32, table.shape, 1)
        slot = lax.broadcasted_iota(jnp.int32, (lot, share), 1)
        first = lax.div(lax.broadcasted_iota(jnp.int32, (lot, share), 0), rows) * depth
        for e in range(experts):
            pick = lane == me.g * experts + e
            scale = jnp.sum(jnp.where(pick, table, 0.0), axis=1, keepdims=True)
            mine_rank = jnp.sum(jnp.where(pick, rank, 0.0), axis=1, keepdims=True)
            hit = jnp.logical_and((slot - first).astype(jnp.float32) == mine_rank, scale > 0.0)
            place[:, e * share:(e + 1) * share] = jnp.where(hit, 1.0, 0.0).astype(place.dtype)
            weigh[:, e * share:(e + 1) * share] = jnp.where(hit, scale, 0.0).astype(weigh.dtype)
        for cols in tiles:
            cols = slice(*cols)
            packed[:, cols] = lax.dot_general(
                place[...], rows_ref[pl.ds(base, lot), cols], (((0,), (0,)), ((), ())),
                preferred_element_type=jnp.float32).astype(packed.dtype)

    def hidden_step(order, s):
        del order
        e, n = lax.div(s, blocks), lax.rem(s, blocks)
        start = pl.multiple_of(e * share, share)
        x = packed[pl.ds(start, share), :]
        gate = jnp.dot(x, wg[s], preferred_element_type=jnp.float32)
        upward = jnp.dot(x, wu[s], preferred_element_type=jnp.float32)
        value = jax.nn.silu(gate) * upward
        hid[pl.ds(start, share), pl.ds(pl.multiple_of(n * TILE, TILE), TILE)] = value.astype(hid.dtype)

    def down_step(order, t):
        base = pl.multiple_of(layers[order] * lot, lot)
        cols = slice(*tiles[t])
        span = slice(0, tiles[t][1] - tiles[t][0])
        for e in range(experts):
            mix = slice(e * share, (e + 1) * share)
            back[mix, span] = jnp.dot(
                hid[mix, :], wd[e * units:(e + 1) * units, cols],
                preferred_element_type=jnp.float32).astype(back.dtype)
        part[pl.ds(base, lot), cols] = jnp.dot(
            weigh[...], back[:, span], preferred_element_type=jnp.float32).astype(part.dtype)

        def make(sem):
            start = pl.multiple_of((layers[order] * 8 + (1 - me.c) * 4) * rows, 4 * rows)
            there = pl.multiple_of(layers[order] * 4 * rows, 4 * rows)
            return remote(
                part.at[pl.ds(start, 4 * rows), cols], mine.at[pl.ds(there, 4 * rows), cols],
                sem, sum_sem.at[layers[order]], device("core"))
        tail = slice(0, width) if t == len(tiles) - 1 else cols
        issue("part", always, 4 * rows if t == len(tiles) - 1 else 0, tail, make)

    def add(size, cols, terms, target, start):
        for at in range(cols.start, cols.stop, TILE):
            piece = slice(at, at + TILE)
            total = None
            for ref, base in terms:
                term = ref[pl.ds(base, size), piece].astype(jnp.float32)
                total = term if total is None else total + term
            target[pl.ds(start, size), piece] = total.astype(target.dtype)

    def own_terms(layer, flip, h=0):
        return [(part, row(me.c, layer, flip, h)), (mine, post(layer, flip, h))]

    def from_core(order):
        start = pl.multiple_of(layers[order] * 4 * rows, 4 * rows)
        landed(mine.at[pl.ds(start, 4 * rows), :], sum_sem.at[layers[order]])

    def two_at(layer, j, h):
        return pl.multiple_of(((layer * 2 + j) * 2 + h) * half, half)

    def one_at(layer, h):
        return pl.multiple_of((layer * 2 + h) * half, half)

    def two_slot(layer, j, h, cols):
        return two.at[pl.ds(two_at(layer, j, h), half), cols]

    def one_slot(layer, h, cols):
        return one.at[pl.ds(one_at(layer, h), half), cols]

    def send_sum(key, cond, layer, flip, h, size, cols, target, recv_sem, where):
        def make(sem):
            return remote(
                mine.at[pl.ds(post(layer(), flip, h), size), cols], target(), sem, recv_sem(), where())
        issue(key, cond, size, cols, make)

    def s_third(order, only=None):
        layer = lambda: layers[order]
        if only != 0:
            from_core(order)
        for j, flips in ((1, lambda h: DIAG), (0, lambda h: FLIPS[1 - h])):
            if only not in (None, j):
                continue
            for h in range(2):
                flip = flips(h)
                add(half, rest, own_terms(layer(), flip, h), mine, post(layer(), flip, h))
                send_sum(
                    "s", always, layer, flip, h, half, rest,
                    lambda j=j, h=h: two_slot(layer(), j, h, rest),
                    lambda j=j, h=h: two_sem.at[layer(), j, h], lambda h=h: device("side", h))

    def s_second(order):
        layer = lambda: layers[order]
        for h in range(2):
            flip = FLIPS[h]
            landed(two_slot(layer(), 1, h, rest), two_sem.at[layer(), 1, h])
            add(half, rest, own_terms(layer(), flip, h) + [(two, two_at(layer(), 1, h))],
                mine, post(layer(), flip, h))
            send_sum(
                "s", always, layer, flip, h, half, rest,
                lambda h=h: one_slot(layer(), h, rest), lambda h=h: one_sem.at[layer(), h],
                lambda h=h: device("near", h))

    def columns_in(layer, h):
        landed(two_slot(layer, 0, h, rest), two_sem.at[layer, 0, h])
        landed(one_slot(layer, h, rest), one_sem.at[layer, h])
        return own_terms(layer, HERE, h) + [(two, two_at(layer, 0, h)), (one, one_at(layer, h))]

    def ways(reach, hop, leap):
        for cond, to, name in (
                (at_layer[hop], reach, "up"), (at_layer[deep - 1 - hop], deep - 1 - reach, "down")):
            over = leap and reach == last and hop == 0
            joins = hop > (1 if leap and reach == last else 0)
            near, z_sem, c_sem = (low, low_sem, clow_sem) if name == "up" else (high, high_sem, chigh_sem)
            yield cond, to, name, over, joins, near, z_sem, c_sem

    def z_sum(reach, hop, only=None):
        for h in (0, 1) if only is None else (only,):
            for cond, to, name, over, joins, near, sem, _ in ways(reach, hop, jump and h == 0):
                def act():
                    terms = columns_in(to, h)
                    if joins:
                        landed(near.at[pl.ds(post(to, HERE, h), half), rest], sem.at[to, h])
                        terms.append((near, post(to, HERE, h)))
                    add(half, rest, terms, mine, post(to, HERE, h))
                pl.when(cond)(act)

                def target(to=to, near=near, over=over, h=h):
                    ref, at = (far, post(0, HERE, h)) if over else (near, post(to, HERE, h))
                    return ref.at[pl.ds(at, half), rest]
                send_sum(
                    ("z sum", name, hop), lambda cond=cond: cond, lambda to=to: to, HERE, h, half,
                    rest, target,
                    lambda to=to, sem=sem, over=over, h=h: far_sem.at[h] if over else sem.at[to, h],
                    lambda to=to, name=name, over=over: (
                        (column(to), me.c) if over else device(name)))

    def c_sum(reach, hop):
        for cond, to, name, _, joins, near, _, sem in ways(reach, hop, False):
            for flip in spots:
                def act():
                    terms = own_terms(to, flip)
                    if joins:
                        landed(near.at[pl.ds(post(to, flip), rows), front], sem.at[column(to, flip)])
                        terms.append((near, post(to, flip)))
                    add(rows, front, terms, mine, post(to, flip))
                pl.when(cond)(act)
                send_sum(
                    ("c sum", name, hop), lambda cond=cond: cond, lambda to=to: to, flip, 0, rows, front,
                    lambda to=to, near=near, flip=flip: near.at[pl.ds(post(to, flip), rows), front],
                    lambda to=to, sem=sem, flip=flip: sem.at[column(to, flip)],
                    lambda name=name: device(name))

    def lined(flip, h, leap):
        beyond = [(low, post(me.z, flip, h)), (high, post(me.z, flip, h))]
        return own_terms(me.z, flip, h) + beyond + ([(far, post(0, flip, h))] if leap else [])

    def z_final():
        for h in range(2):
            terms = columns_in(me.z, h)[2:] + lined(HERE, h, jump and h == 0)
            spot = pl.ds(post(me.z, HERE, h), half)
            pl.when(me.below)(lambda: landed(low.at[spot, rest], low_sem.at[me.z, h]))
            pl.when(me.above)(lambda: landed(high.at[spot, rest], high_sem.at[me.z, h]))
            if jump and h == 0:
                spot_far = pl.ds(post(0, HERE, h), half)
                pl.when(me.end)(lambda: landed(far.at[spot_far, rest], far_sem.at[h]))
            add(half, rest, terms, out_ref, h * half)

    def c_back():
        for flip in (DIAG,) + FLIPS + (HERE,):
            g = column(me.z, flip)
            spot = pl.ds(post(me.z, flip), rows)
            pl.when(me.below)(lambda: landed(low.at[spot, front], clow_sem.at[g]))
            pl.when(me.above)(lambda: landed(high.at[spot, front], chigh_sem.at[g]))
        for j, flips in ((1, lambda h: DIAG), (0, lambda h: FLIPS[1 - h])):
            for h in range(2):
                flip = flips(h)
                add(half, front, lined(flip, h, False), mine, post(me.z, flip, h))
                send_sum(
                    "c sum", always, own, flip, h, half, front,
                    lambda j=j, h=h: two_slot(me.z, j, h, front),
                    lambda j=j, h=h: xtwo_sem.at[j, h], lambda h=h: device("side", h))

    def c_cross():
        for h in range(2):
            flip = FLIPS[h]
            landed(two_slot(me.z, 1, h, front), xtwo_sem.at[1, h])
            add(half, front, lined(flip, h, False) + [(two, two_at(me.z, 1, h))], mine, post(me.z, flip, h))
            send_sum(
                "c sum", always, own, flip, h, half, front, lambda h=h: one_slot(me.z, h, front),
                lambda h=h: xone_sem.at[h], lambda h=h: device("near", h))

    def c_final():
        for h in range(2):
            landed(two_slot(me.z, 0, h, front), xtwo_sem.at[0, h])
            landed(one_slot(me.z, h, front), xone_sem.at[h])
            add(half, front, lined(HERE, h, False) + [(two, two_at(me.z, 0, h)), (one, one_at(me.z, h))],
                out_ref, h * half)

    def clear(ref, layer):
        base = layer * 4 * rows

        def body(i, carry):
            ref[pl.ds(pl.multiple_of(base + i * half, half), half), :] = jnp.zeros((half, width), ref.dtype)
            return carry
        lax.fori_loop(0, 8, body, None)

    do = dict(
        z_first=z_first, z_cross=z_cross, z_second=z_second, z_third=z_third, c_first=c_first, c_second=c_second,
        c_third=c_third, c_line=c_line, turn_down=turn_down, s_third=s_third, s_second=s_second,
        z_sum=z_sum, c_sum=c_sum, z_final=z_final, c_back=c_back, c_cross=c_cross, c_final=c_final,
        weights=weights,
        clear_low=lambda: pl.when(jnp.logical_not(me.below))(lambda: clear(low, me.z)),
        clear_high=lambda: pl.when(jnp.logical_not(me.above))(lambda: clear(high, me.z)),
        clear_far=lambda: pl.when(jnp.logical_not(me.end))(lambda: clear(far, 0)))
    before, plan, after = order_of_work(deep, experts)

    def run(acts):
        for name, *args in acts:
            do[name](*args)

    own_copy.wait()
    run(before)
    for kind, ref in enumerate((wg, wu)):
        pltpu.make_async_copy(ref, ref, weight_sem.at[kind]).wait()
    subs = experts * blocks
    for order in range(deep):
        other_core(order)
        acts = plan[order]
        run(acts.get(-1, []))
        pack(order)

        def body(s, carry, order=order, acts=acts):
            for k in range(subs):
                if acts.get(k):
                    pl.when(s == k)(lambda k=k: run(acts[k]))
            hidden_step(order, s)
            return carry
        lax.fori_loop(0, subs, body, None)
        for t in range(len(tiles)):
            run(acts.get(subs + t, []))
            down_step(order, t)
    run(after)
    assert len(sends) == send_sem.shape[0], len(sends)
    for number, cond, total, cols in sends.values():
        spent = rows_ref.at[pl.ds(0, total), cols]
        when(cond(), lambda: remote(
            spent, spent, send_sem.at[number], own_sem, (me.g, 1 - me.c)).wait_send())


def order_of_work(deep, experts):
    last = deep - 1
    before = [("c_first",), ("z_first", 0), ("z_cross", 0), ("weights",)]
    before += [("clear_low",), ("clear_high",), ("clear_far",)]
    before += [("c_second",), ("turn_down", 0)]
    before += [("z_second", 0), ("z_first", 1), ("z_cross", 1)]
    before += [("turn_down", e) for e in range(1, experts)]
    before += [("c_third",), ("z_third", 0)]
    plan = [{} for _ in range(deep)]

    def put(order, step, *acts):
        plan[min(order, last)].setdefault(step, []).extend(acts)

    put(0, 1, ("z_second", 1))
    for order in range(last):
        if order:
            put(*((1, -1) if order == 1 else (order - 1, 7)), ("z_second", order + 1))
        if order + 2 < deep:
            put(order, 0 if order else 2, ("z_first", order + 2), ("z_cross", order + 2))
        put(order, (2, 5, 4)[order] if deep == 4 else 2, ("c_line", order + 1))
        put(order, (6, 5, 5)[order] if deep == 4 else 5, ("z_third", order + 1))
    if last > 1:
        put(last - 1, 0, ("s_third", 1), ("c_sum", 1, 0))
        for order in range(2, last):
            put(last, 7, ("s_second", order))
        put(last, 7, ("z_sum", 1, 0, 0))
        put(last, -1, ("s_second", 1))
        for order in range(2, last):
            put(last, 0, ("s_third", order), ("c_sum", order, 0))
    else:
        put(last, 0, ("s_third", 0))
    after = [("s_third", last), ("c_sum", last, 0)]
    after += [("c_sum", reach, hop) for reach in range(2, last) for hop in range(1, reach)]
    after += [("c_sum", last, hop) for hop in range(1, 2 if last > 1 else 1)]
    after += [("s_second", last)]
    if last > 1:
        after += [("s_third", 0)]
    after += [("z_sum", reach, 0) for reach in range(2, last)]
    after += [("z_sum", last, 0, 1), ("z_sum", last, 0, 0)]
    if last > 1:
        after += [("z_sum", 1, 0, 1)]
    after += [("c_sum", last, hop) for hop in range(2, last)]
    after += [("z_sum", last, hop, 0) for hop in range(1, 2 if last > 1 else 1)]
    after += [("z_sum", last, hop, 1) for hop in range(1, 2 if last > 1 else 1)]
    after += [("z_sum", reach, hop) for reach in range(2, last) for hop in range(1, reach)]
    after += [("s_second", 0), ("c_back",)]
    after += [("z_sum", last, hop, h) for hop in range(2, last) for h in range(2)]
    after += [("c_cross",), ("z_final",), ("c_final",)]
    return before, plan, after


def fused_body(tokens, gate_weights, expert_ids, w_gate, w_up, w_down):
    columns = lax.axis_size("grp")
    rows, width = tokens.shape
    experts, _, units = w_gate.shape
    deep = columns // 4
    half = rows // 2
    split = max(1, round(width * 2 / 9 / TILE)) * TILE
    split_back = split
    edges = list(range(0, width, 4 * TILE)) + [width]
    tiles = list(zip(edges[:-1], edges[1:]))
    padded = -(-columns * experts // LANES) * LANES
    blocks = units // TILE
    bf16 = tokens.dtype
    depth = 2 * rows * RGROUPS // (columns * experts)
    dma = pltpu.SemaphoreType.DMA
    vmem = lambda *shape: pltpu.VMEM(shape, bf16)
    anywhere = pl.BlockSpec(memory_space=pl.ANY)
    local = pl.BlockSpec(memory_space=pltpu.VMEM)
    lined = columns * rows
    groups = 8 * (deep - 1) + 2 * (deep - 2) + 7
    return pl.pallas_call(
        functools.partial(layer_kernel, columns, split, split_back, depth, tiles),
        out_shape=jax.ShapeDtypeStruct((rows, width), bf16),
        in_specs=[anywhere, local, local, anywhere, anywhere, anywhere],
        out_specs=local,
        scratch_shapes=[
            vmem(2 * lined, width + padded),
            vmem(experts * blocks, width, TILE), vmem(experts * blocks, width, TILE),
            vmem(experts * units, width),
            vmem(8 * rows, experts * 8 * depth), vmem(8 * rows, experts * 8 * depth),
            vmem(experts * 8 * depth, width), vmem(experts * 8 * depth, units),
            vmem(experts * 8 * depth, 4 * TILE),
            vmem(2 * lined, width), vmem(lined, width),
            vmem(deep * 4 * half, width), vmem(deep * rows, width),
            vmem(lined, width), vmem(lined, width),
            vmem(4 * rows, width),
            dma, dma((2,)), dma((experts,)), dma((groups,)), dma((2, columns)), dma((columns,)), dma((2,)),
            dma((deep,)), dma((deep,)), dma((deep, 2, 2)), dma((deep, 2)), dma((deep, 2)), dma((deep, 2)),
            dma((2,)), dma((2, 2)), dma((2,)), dma((columns,)), dma((columns,)),
        ],
        compiler_params=pltpu.CompilerParams(
            collective_id=1, has_side_effects=True, vmem_limit_bytes=54 * 2**20),
        name="expert_layer",
    )(tokens, expert_ids.T, gate_weights.T, w_gate, w_up, w_down)


def expert_rows(inputs, scales, gate_part, up_part, down_part):
    gate_act = jnp.dot(inputs, gate_part, preferred_element_type=jnp.float32)
    upward = jnp.dot(inputs, up_part, preferred_element_type=jnp.float32)
    hidden = (jax.nn.silu(gate_act) * upward).astype(jnp.bfloat16)
    projected = lax.dot_general(
        hidden, down_part, (((1,), (1,)), ((), ())), preferred_element_type=jnp.float32
    )
    return projected * scales.astype(jnp.float32)[:, None]


def weights_path(rows_in, scales_in, w_gate, w_up, w_down):
    row_dims = rows_in.shape
    shard_units = w_gate.shape[2]
    expert_inputs = [rows_in[:, expert].reshape(-1, row_dims[3]) for expert in range(row_dims[1])]
    expert_scales = [scales_in[:, expert].reshape(-1) for expert in range(row_dims[1])]
    starting = tuple(
        (
            jnp.zeros((row_dims[0] * row_dims[2], row_dims[3]), jnp.float32)
            for expert in range(row_dims[1])
        )
    )
    gate_piece = lax.all_gather(w_gate, "loc", axis=2, tiled=True)
    up_piece = lax.all_gather(w_up, "loc", axis=2, tiled=True)
    down_piece = lax.all_gather(w_down, "loc", axis=2, tiled=True)
    updated = []
    for expert in range(row_dims[1]):
        running = starting[expert]
        for block_index in range(gate_piece.shape[2] // shard_units):
            lower_unit = block_index * shard_units
            upper_unit = lower_unit + shard_units
            values = expert_rows(
                expert_inputs[expert],
                expert_scales[expert],
                gate_piece[expert][:, lower_unit:upper_unit],
                up_piece[expert][:, lower_unit:upper_unit],
                down_piece[expert][:, lower_unit:upper_unit],
            )
            rounded = lax.optimization_barrier(values.astype(jnp.bfloat16))
            running = running + rounded.astype(jnp.float32)
        updated.append(running)
    folded = tuple(updated)
    stacked = jnp.stack(
        [folded_part.reshape(row_dims[0], row_dims[2], row_dims[3]) for folded_part in folded],
        axis=1,
    )
    return stacked.astype(jnp.bfloat16)


def slot_body(tokens, gate_weights, expert_ids, w_gate, w_up, w_down):
    tok_count = tokens.shape[0]
    choices_per = expert_ids.shape[1]
    feature_count = tokens.shape[1]
    group_count = lax.axis_size("grp")
    local_experts = w_gate.shape[0]
    expert_total = group_count * local_experts
    slot_depth = 2 * tok_count * RGROUPS // expert_total
    slot_total = expert_total * slot_depth
    pair_ids = expert_ids.reshape(-1)
    pair_count = pair_ids.shape[0]
    pair_order = jnp.arange(pair_count, dtype=jnp.int32)
    same_expert = (pair_ids[:, None] == pair_ids[None, :]).astype(jnp.int32)
    earlier = (pair_order[:, None] > pair_order[None, :]).astype(jnp.int32)
    slot_rank = jnp.sum(same_expert * earlier, axis=1)
    position = pair_ids * slot_depth + slot_rank
    pair_onehot = jnp.arange(slot_total, dtype=jnp.int32)[:, None] == position[None, :]
    placement = jnp.sum(
        pair_onehot.reshape(slot_total, tok_count, choices_per).astype(jnp.int32), axis=2
    ).astype(jnp.bfloat16)
    send_rows = jnp.dot(placement, tokens, preferred_element_type=jnp.float32).astype(jnp.bfloat16)
    flat_scales = gate_weights.reshape(-1).astype(jnp.float32)
    send_scales = jnp.sum(jnp.where(pair_onehot, flat_scales[None, :], 0.0), axis=1).astype(
        jnp.bfloat16
    )
    send_rows = send_rows.reshape(group_count, local_experts, slot_depth, feature_count)
    send_scales = send_scales.reshape(group_count, local_experts, slot_depth)
    computed = weights_path(
        lax.all_to_all(send_rows, "grp", split_axis=0, concat_axis=0, tiled=True),
        lax.all_to_all(send_scales, "grp", split_axis=0, concat_axis=0, tiled=True),
        w_gate,
        w_up,
        w_down,
    )
    returned = lax.all_to_all(computed, "grp", split_axis=0, concat_axis=0, tiled=True)
    flat_back = returned.reshape(slot_total, feature_count)
    mixed_out = lax.dot_general(
        placement, flat_back, (((0,), (0,)), ((), ())), preferred_element_type=jnp.float32
    )
    return mixed_out.astype(jnp.bfloat16)


def body(tokens, gate_weights, expert_ids, w_gate, w_up, w_down):
    tok_count, width = tokens.shape
    units = w_gate.shape[2]
    columns = lax.axis_size("grp")
    slot_depth = 2 * tok_count * RGROUPS // (columns * w_gate.shape[0])
    dense = slot_depth * w_gate.shape[0] >= tok_count
    fits = (columns % 4 == 0 and lax.axis_size("loc") == 2 and tok_count % 32 == 0
            and columns >= 8 and width % TILE == 0 and width > TILE
            and units % TILE == 0 and width % units == 0 and 8 * slot_depth % LANES == 0)
    chosen = fused_body if dense and fits else slot_body
    return chosen(tokens, gate_weights, expert_ids, w_gate, w_up, w_down)


def solution(mesh):
    placed = (
        P(("grp", "loc"), None),
        P(("grp", "loc"), None),
        P(("grp", "loc"), None),
        P("grp", None, "loc"),
        P("grp", None, "loc"),
        P("grp", None, "loc"),
    )
    return jax.shard_map(
        body, mesh=mesh, in_specs=placed, out_specs=P(("grp", "loc"), None), check_vma=False
    )
```

```python
import functools

import jax
import jax.numpy as jnp
from jax import lax
from jax.experimental import pallas as pl
from jax.experimental.pallas import tpu as pltpu
from jax.sharding import PartitionSpec as P

RGROUPS = 8
LANES = 128
TILE = 256
MESH = pl.DeviceIdType.MESH
FLIPS = ((1, 0), (0, 1))
HERE, DIAG = (0, 0), (1, 1)


class Place:
    def __init__(self, columns):
        self.deep = columns // 4
        self.g = lax.axis_index("grp")
        self.c = lax.axis_index("loc")
        self.x = lax.rem(self.g, 2)
        self.y = lax.rem(lax.div(self.g, 2), 2)
        self.z = lax.div(self.g, 4)
        self.below = self.z > 0
        self.above = self.z < self.deep - 1
        self.end = jnp.logical_or(self.z == 0, self.z == self.deep - 1)

    def spot(self, flip):
        x = 1 - self.x if flip[0] else self.x
        y = 1 - self.y if flip[1] else self.y
        return y * 2 + x

    def at(self, dz=0, flip=HERE):
        return (self.z + dz) * 4 + self.spot(flip)

    def line(self, step):
        if step == 0:
            return [(0, None)]
        return [(-step, self.z >= step), (step, self.z + step < self.deep)]

    def layer(self, order):
        picked = self.z
        for z in range(self.deep):
            ranked = sorted(range(self.deep), key=lambda other: (abs(other - z), other))
            picked = jnp.where(self.z == z, ranked[order], picked)
        return picked


def when(cond, act):
    if cond is None:
        act()
    else:
        pl.when(cond)(act)


def both(a, b):
    return b if a is None else jnp.logical_and(a, b)


def greet(me):
    barrier = pltpu.get_barrier_semaphore()
    partners = [
        (None, me.at(0, (1, 0)), me.c),
        (None, me.at(0, (0, 1)), me.c),
        (None, me.g, 1 - me.c),
        (me.below, me.at(-1), me.c),
        (me.above, me.at(1), me.c),
    ]
    for cond, g, c in partners:
        when(cond, lambda g=g, c=c: pl.semaphore_signal(
            barrier, inc=1, device_id=(g, c), device_id_type=MESH))
    edges = (me.z > 0).astype(jnp.int32) + (me.z < me.deep - 1).astype(jnp.int32)
    pl.semaphore_wait(barrier, 3 + edges)


def layer_kernel(columns, split, split_back, depth, tiles, tokens_hbm, ids_ref, gains_ref, wg_hbm, wu_hbm, wd_hbm, out_ref,
                 rows_ref, wg, wu, wd, place, weigh, packed, hid, back, part, mine, two, one, low, high,
                 far, own_sem, weight_sem, down_sem, send_sem, gz_ici, gc_ici, gc_half, core_sem,
                 sum_sem, two_sem, one_sem, low_sem, high_sem, far_sem,
                 xtwo_sem, xone_sem, clow_sem, chigh_sem):
    me = Place(columns)
    deep = me.deep
    rows, width = tokens_hbm.shape
    half = rows // 2
    lot = 8 * rows
    experts, _, units = wd_hbm.shape
    blocks = units // TILE
    lines = [me.line(step) for step in range(deep)]
    layers = [me.layer(order) for order in range(deep)]
    at_layer = [me.z == layer for layer in range(deep)]
    direct = slice(0, split)
    front, rest = slice(0, split_back), slice(split_back, width)
    carried = slice(split, rows_ref.shape[1])
    spots = (HERE,) + FLIPS + (DIAG,)
    sends = {}
    last = deep - 1
    jump = deep > 2

    own_rows = pl.multiple_of((me.z * 8 + me.c * 4 + me.spot(HERE)) * rows, rows)
    own_copy = pltpu.make_async_copy(
        tokens_hbm, rows_ref.at[pl.ds(own_rows, rows), 0:width], own_sem)
    own_copy.start()

    def weights():
        for e in range(experts):
            for b in range(width // units):
                pltpu.make_async_copy(
                    wd_hbm.at[e, b * units:(b + 1) * units, :],
                    wd.at[e * units:(e + 1) * units, b * units:(b + 1) * units], down_sem.at[e]).start()
        for s in range(experts * blocks):
            e, n = divmod(s, blocks)
            for kind, (source, target) in enumerate(((wg_hbm, wg), (wu_hbm, wu))):
                pltpu.make_async_copy(
                    source.at[e, :, n * TILE:(n + 1) * TILE], target.at[s], weight_sem.at[kind]).start()

    numbers = lax.broadcasted_iota(jnp.int32, (rows_ref.shape[1] - width, rows), 0)
    table = jnp.zeros(numbers.shape, jnp.float32)
    gains = gains_ref[...].astype(jnp.float32)
    ids = ids_ref[...]
    for k in range(ids.shape[0]):
        table = table + jnp.where(ids[k:k + 1, :] == numbers, gains[k:k + 1, :], 0.0)
    table = table.astype(rows_ref.dtype)
    unit = (lax.broadcasted_iota(jnp.int32, (rows, rows), 0)
            == lax.broadcasted_iota(jnp.int32, (rows, rows), 1)).astype(rows_ref.dtype)
    rows_ref[pl.ds(own_rows, rows), width:] = lax.dot_general(
        unit, table, (((1,), (1,)), ((), ())), preferred_element_type=jnp.float32).astype(rows_ref.dtype)
    greet(me)

    def row(c, layer, flip=HERE, h=0):
        return pl.multiple_of((layer * 8 + c * 4 + me.spot(flip)) * rows + h * half, half)

    def post(layer, flip=HERE, h=0):
        return pl.multiple_of((layer * 4 + me.spot(flip)) * rows + h * half, half)

    def column(layer, flip=HERE):
        return layer * 4 + me.spot(flip)

    def device(kind, h=0):
        return {
            "up": lambda: (me.at(1), me.c),
            "down": lambda: (me.at(-1), me.c),
            "near": lambda: (me.at(0, FLIPS[h]), me.c),
            "side": lambda: (me.at(0, FLIPS[1 - h]), me.c),
            "core": lambda: (me.g, 1 - me.c),
        }[kind]()

    def remote(source, target, send_sem, recv_sem, where):
        return pltpu.make_async_remote_copy(
            src_ref=source, dst_ref=target, send_sem=send_sem, recv_sem=recv_sem,
            device_id=where, device_id_type=MESH)

    def issue(key, cond, size, cols, make):
        number, _, total, _ = sends.get(key, (len(sends), cond, 0, cols))
        sends[key] = (number, cond, total + size, cols)
        when(cond(), lambda: make(send_sem.at[number]).start())

    def landed(ref, sem):
        remote(ref, ref, own_sem, sem, (me.g, 1 - me.c)).wait_recv()

    def always():
        return None

    def z_slot(h, layer, flip):
        return rows_ref.at[pl.ds(row(me.c, layer, flip, h), half), carried]

    def push_z(key, cond, h, layer, flip, kind):
        def make(sem):
            slot = z_slot(h, layer(), flip)
            recv = core_sem.at[layer()] if kind == "core" else gz_ici.at[h, column(layer(), flip)]
            return remote(slot, slot, sem, recv, device(kind, h))
        issue(key, cond, half, carried, make)

    def z_landed(h, layer, flip):
        landed(z_slot(h, layer, flip), gz_ici.at[h, column(layer, flip)])

    def c_slot(layer, flip, h=None):
        size = rows if h is None else half
        return rows_ref.at[pl.ds(row(me.c, layer, flip, h or 0), size), direct]

    def push_c(key, cond, layer, flip, kind, h=None, k=0):
        size = rows if h is None else half

        def make(sem):
            slot = c_slot(layer(), flip, h)
            recv = (core_sem.at[layer()] if kind == "core"
                    else gc_ici.at[column(layer(), flip)] if h is None else gc_half.at[h])
            return remote(slot, slot, sem, recv, device(kind, k))
        issue(key, cond, size, direct, make)

    def z_first(step):
        for dz, cond in lines[step]:
            layer = lambda dz=dz: me.z + dz
            for h in range(2):
                if step:
                    when(cond, lambda: z_landed(h, layer(), HERE))
                if dz <= 0 and step < last:
                    push_z(("up", dz), lambda cond=cond: both(cond, me.above), h, layer, HERE, "up")
                if dz >= 0 and step < last:
                    push_z(("down", dz), lambda cond=cond: both(cond, me.below), h, layer, HERE, "down")

    def z_cross(order):
        for kind in ("near", "side", "core"):
            for h in range(2):
                push_z("z", always, h, lambda: layers[order], HERE, kind)

    def z_second(order):
        for h in range(2):
            z_landed(h, layers[order], FLIPS[h])
            push_z("z", always, h, lambda: layers[order], FLIPS[h], "side")
            push_z("z", always, h, lambda: layers[order], FLIPS[h], "core")

    def z_third(order):
        for flips in (lambda h: FLIPS[1 - h], lambda h: DIAG):
            for h in range(2):
                z_landed(h, layers[order], flips(h))
                push_z("z", always, h, lambda: layers[order], flips(h), "core")

    def own():
        return me.z

    def along(flip):
        push_c("c up", lambda: me.above, own, flip, "up")
        push_c("c down", lambda: me.below, own, flip, "down")
        push_c("c", always, own, flip, "core")

    def c_first():
        for k in range(2):
            push_c("c", always, own, HERE, "near" if k == 0 else "side")
        along(HERE)

    def c_second():
        for k in range(2):
            landed(c_slot(me.z, FLIPS[k]), gc_ici.at[me.at(0, FLIPS[k])])
            push_c("c", always, own, FLIPS[k], "side", h=k, k=k)
            along(FLIPS[k])

    def c_third():
        for h in range(2):
            landed(c_slot(me.z, DIAG, h), gc_half.at[h])
        along(DIAG)

    def c_line(step):
        for dz, cond in lines[step]:
            layer = lambda dz=dz: me.z + dz
            for flip in spots:
                when(cond, lambda: landed(c_slot(layer(), flip), gc_ici.at[column(layer(), flip)]))
                if step < last:
                    edge, kind = (me.above, "up") if dz < 0 else (me.below, "down")
                    push_c(("c on", dz), lambda cond=cond, edge=edge: both(cond, edge), layer, flip, kind)
                push_c(("c in", dz), lambda cond=cond: cond, layer, flip, "core")

    def other_core(order):
        base = pl.multiple_of((layers[order] * 8 + (1 - me.c) * 4) * rows, 4 * rows)
        landed(rows_ref.at[pl.ds(base, 4 * rows), :], core_sem.at[layers[order]])

    def turn_down(e):
        whole = wd.at[e * units:(e + 1) * units, :]
        pltpu.make_async_copy(whole, whole, down_sem.at[e]).wait()
        for b in range(width // units):
            block = (slice(e * units, (e + 1) * units), slice(b * units, (b + 1) * units))
            wd[block] = wd[block].T

    share = 8 * depth

    def pack(order):
        base = pl.multiple_of(layers[order] * lot, lot)
        table = rows_ref[pl.ds(base, lot), width:].astype(jnp.float32)
        token = lax.broadcasted_iota(jnp.int32, (lot, lot), 0)
        other = lax.broadcasted_iota(jnp.int32, (lot, lot), 1)
        earlier = jnp.logical_and(other < token, lax.div(other, rows) == lax.div(token, rows))
        rank = jnp.dot(
            jnp.where(earlier, 1.0, 0.0).astype(place.dtype),
            jnp.where(table > 0.0, 1.0, 0.0).astype(place.dtype), preferred_element_type=jnp.float32)
        lane = lax.broadcasted_iota(jnp.int32, table.shape, 1)
        slot = lax.broadcasted_iota(jnp.int32, (lot, share), 1)
        first = lax.div(lax.broadcasted_iota(jnp.int32, (lot, share), 0), rows) * depth
        for e in range(experts):
            pick = lane == me.g * experts + e
            scale = jnp.sum(jnp.where(pick, table, 0.0), axis=1, keepdims=True)
            mine_rank = jnp.sum(jnp.where(pick, rank, 0.0), axis=1, keepdims=True)
            hit = jnp.logical_and((slot - first).astype(jnp.float32) == mine_rank, scale > 0.0)
            place[:, e * share:(e + 1) * share] = jnp.where(hit, 1.0, 0.0).astype(place.dtype)
            weigh[:, e * share:(e + 1) * share] = jnp.where(hit, scale, 0.0).astype(weigh.dtype)
        for cols in tiles:
            cols = slice(*cols)
            packed[:, cols] = lax.dot_general(
                place[...], rows_ref[pl.ds(base, lot), cols], (((0,), (0,)), ((), ())),
                preferred_element_type=jnp.float32).astype(packed.dtype)

    def hidden_step(order, s):
        del order
        e, n = lax.div(s, blocks), lax.rem(s, blocks)
        start = pl.multiple_of(e * share, share)
        x = packed[pl.ds(start, share), :]
        gate = jnp.dot(x, wg[s], preferred_element_type=jnp.float32)
        upward = jnp.dot(x, wu[s], preferred_element_type=jnp.float32)
        value = jax.nn.silu(gate) * upward
        hid[pl.ds(start, share), pl.ds(pl.multiple_of(n * TILE, TILE), TILE)] = value.astype(hid.dtype)

    def down_step(order, t):
        base = pl.multiple_of(layers[order] * lot, lot)
        cols = slice(*tiles[t])
        span = slice(0, tiles[t][1] - tiles[t][0])
        for e in range(experts):
            mix = slice(e * share, (e + 1) * share)
            back[mix, span] = jnp.dot(
                hid[mix, :], wd[e * units:(e + 1) * units, cols],
                preferred_element_type=jnp.float32).astype(back.dtype)
        part[pl.ds(base, lot), cols] = jnp.dot(
            weigh[...], back[:, span], preferred_element_type=jnp.float32).astype(part.dtype)

        def make(sem):
            start = pl.multiple_of((layers[order] * 8 + (1 - me.c) * 4) * rows, 4 * rows)
            there = pl.multiple_of(layers[order] * 4 * rows, 4 * rows)
            return remote(
                part.at[pl.ds(start, 4 * rows), cols], mine.at[pl.ds(there, 4 * rows), cols],
                sem, sum_sem.at[layers[order]], device("core"))
        tail = slice(0, width) if t == len(tiles) - 1 else cols
        issue("part", always, 4 * rows if t == len(tiles) - 1 else 0, tail, make)

    def add(size, cols, terms, target, start):
        for at in range(cols.start, cols.stop, TILE):
            piece = slice(at, at + TILE)
            total = None
            for ref, base in terms:
                term = ref[pl.ds(base, size), piece].astype(jnp.float32)
                total = term if total is None else total + term
            target[pl.ds(start, size), piece] = total.astype(target.dtype)

    def own_terms(layer, flip, h=0):
        return [(part, row(me.c, layer, flip, h)), (mine, post(layer, flip, h))]

    def from_core(order):
        start = pl.multiple_of(layers[order] * 4 * rows, 4 * rows)
        landed(mine.at[pl.ds(start, 4 * rows), :], sum_sem.at[layers[order]])

    def two_at(layer, j, h):
        return pl.multiple_of(((layer * 2 + j) * 2 + h) * half, half)

    def one_at(layer, h):
        return pl.multiple_of((layer * 2 + h) * half, half)

    def two_slot(layer, j, h, cols):
        return two.at[pl.ds(two_at(layer, j, h), half), cols]

    def one_slot(layer, h, cols):
        return one.at[pl.ds(one_at(layer, h), half), cols]

    def send_sum(key, cond, layer, flip, h, size, cols, target, recv_sem, where, spent=None):
        def make(sem):
            return remote(
                mine.at[pl.ds(post(layer(), flip, h), size), cols], target(), sem, recv_sem(), where())
        issue(key, cond, *(spent or (size, cols)), make)

    def s_third(order, only=None):
        layer = lambda: layers[order]
        if only != 0:
            from_core(order)
        for j, flips in ((1, lambda h: DIAG), (0, lambda h: FLIPS[1 - h])):
            if only not in (None, j):
                continue
            for h in range(2):
                flip = flips(h)
                add(half, rest, own_terms(layer(), flip, h), mine, post(layer(), flip, h))
                send_sum(
                    "s", always, layer, flip, h, half, rest,
                    lambda j=j, h=h: two_slot(layer(), j, h, rest),
                    lambda j=j, h=h: two_sem.at[layer(), j, h], lambda h=h: device("side", h))

    def s_second(order):
        layer = lambda: layers[order]
        for h in range(2):
            flip = FLIPS[h]
            landed(two_slot(layer(), 1, h, rest), two_sem.at[layer(), 1, h])
            add(half, rest, own_terms(layer(), flip, h) + [(two, two_at(layer(), 1, h))],
                mine, post(layer(), flip, h))
            send_sum(
                "s", always, layer, flip, h, half, rest,
                lambda h=h: one_slot(layer(), h, rest), lambda h=h: one_sem.at[layer(), h],
                lambda h=h: device("near", h))

    def columns_in(layer, h, wait):
        if wait:
            landed(two_slot(layer, 0, h, rest), two_sem.at[layer, 0, h])
            landed(one_slot(layer, h, rest), one_sem.at[layer, h])
        return own_terms(layer, HERE, h) + [(two, two_at(layer, 0, h)), (one, one_at(layer, h))]

    def ways(reach, hop, leap):
        for cond, to, name in (
                (at_layer[hop], reach, "up"), (at_layer[deep - 1 - hop], deep - 1 - reach, "down")):
            over = leap and reach == last and hop == 0
            joins = hop > (1 if leap and reach == last else 0)
            near, z_sem, c_sem = (low, low_sem, clow_sem) if name == "up" else (high, high_sem, chigh_sem)
            yield cond, to, name, over, joins, near, z_sem, c_sem

    middle = split_back + (width - split_back) // (2 * TILE) * TILE
    parts = (slice(split_back, middle), slice(middle, width))

    def z_sum(reach, hop, only=None):
        for h in (0, 1) if only is None else (only,):
            for cond, to, name, over, joins, near, sem, _ in ways(reach, hop, jump and h == 0):
                for p, cols in enumerate(parts):
                    def act():
                        terms = columns_in(to, h, p == 0)
                        if joins:
                            landed(near.at[pl.ds(post(to, HERE, h), half), cols], sem.at[to, h, p])
                            terms.append((near, post(to, HERE, h)))
                        add(half, cols, terms, mine, post(to, HERE, h))
                    pl.when(cond)(act)

                    def target(to=to, near=near, over=over, h=h, cols=cols):
                        ref, at = (far, post(0, HERE, h)) if over else (near, post(to, HERE, h))
                        return ref.at[pl.ds(at, half), cols]
                    send_sum(
                        ("z sum", name, hop), lambda cond=cond: cond, lambda to=to: to, HERE, h, half,
                        cols, target,
                        lambda to=to, sem=sem, over=over, h=h, p=p: (
                            far_sem.at[p] if over else sem.at[to, h, p]),
                        lambda to=to, name=name, over=over: (
                            (column(to), me.c) if over else device(name)),
                        spent=(half if p else 0, rest))

    def c_sum(reach, hop):
        for cond, to, name, _, joins, near, _, sem in ways(reach, hop, False):
            for flip in spots:
                def act():
                    terms = own_terms(to, flip)
                    if joins:
                        landed(near.at[pl.ds(post(to, flip), rows), front], sem.at[column(to, flip)])
                        terms.append((near, post(to, flip)))
                    add(rows, front, terms, mine, post(to, flip))
                pl.when(cond)(act)
                send_sum(
                    ("c sum", name, hop), lambda cond=cond: cond, lambda to=to: to, flip, 0, rows, front,
                    lambda to=to, near=near, flip=flip: near.at[pl.ds(post(to, flip), rows), front],
                    lambda to=to, sem=sem, flip=flip: sem.at[column(to, flip)],
                    lambda name=name: device(name))

    def lined(flip, h, leap):
        beyond = [(low, post(me.z, flip, h)), (high, post(me.z, flip, h))]
        return own_terms(me.z, flip, h) + beyond + ([(far, post(0, flip, h))] if leap else [])

    def z_final():
        for h in range(2):
            spot = pl.ds(post(me.z, HERE, h), half)
            spot_far = pl.ds(post(0, HERE, h), half)
            for p, cols in enumerate(parts):
                terms = columns_in(me.z, h, p == 0)[2:] + lined(HERE, h, jump and h == 0)
                pl.when(me.below)(lambda: landed(low.at[spot, cols], low_sem.at[me.z, h, p]))
                pl.when(me.above)(lambda: landed(high.at[spot, cols], high_sem.at[me.z, h, p]))
                if jump and h == 0:
                    pl.when(me.end)(lambda: landed(far.at[spot_far, cols], far_sem.at[p]))
                add(half, cols, terms, out_ref, h * half)

    def c_back():
        for flip in (DIAG,) + FLIPS + (HERE,):
            g = column(me.z, flip)
            spot = pl.ds(post(me.z, flip), rows)
            pl.when(me.below)(lambda: landed(low.at[spot, front], clow_sem.at[g]))
            pl.when(me.above)(lambda: landed(high.at[spot, front], chigh_sem.at[g]))
        for j, flips in ((1, lambda h: DIAG), (0, lambda h: FLIPS[1 - h])):
            for h in range(2):
                flip = flips(h)
                add(half, front, lined(flip, h, False), mine, post(me.z, flip, h))
                send_sum(
                    "c sum", always, own, flip, h, half, front,
                    lambda j=j, h=h: two_slot(me.z, j, h, front),
                    lambda j=j, h=h: xtwo_sem.at[j, h], lambda h=h: device("side", h))

    def c_cross():
        for h in range(2):
            flip = FLIPS[h]
            landed(two_slot(me.z, 1, h, front), xtwo_sem.at[1, h])
            add(half, front, lined(flip, h, False) + [(two, two_at(me.z, 1, h))], mine, post(me.z, flip, h))
            send_sum(
                "c sum", always, own, flip, h, half, front, lambda h=h: one_slot(me.z, h, front),
                lambda h=h: xone_sem.at[h], lambda h=h: device("near", h))

    def c_final():
        for h in range(2):
            landed(two_slot(me.z, 0, h, front), xtwo_sem.at[0, h])
            landed(one_slot(me.z, h, front), xone_sem.at[h])
            add(half, front, lined(HERE, h, False) + [(two, two_at(me.z, 0, h)), (one, one_at(me.z, h))],
                out_ref, h * half)

    def clear(ref, layer):
        base = layer * 4 * rows

        def body(i, carry):
            ref[pl.ds(pl.multiple_of(base + i * half, half), half), :] = jnp.zeros((half, width), ref.dtype)
            return carry
        lax.fori_loop(0, 8, body, None)

    do = dict(
        z_first=z_first, z_cross=z_cross, z_second=z_second, z_third=z_third, c_first=c_first, c_second=c_second,
        c_third=c_third, c_line=c_line, turn_down=turn_down, s_third=s_third, s_second=s_second,
        z_sum=z_sum, c_sum=c_sum, z_final=z_final, c_back=c_back, c_cross=c_cross, c_final=c_final,
        weights=weights,
        clear_low=lambda: pl.when(jnp.logical_not(me.below))(lambda: clear(low, me.z)),
        clear_high=lambda: pl.when(jnp.logical_not(me.above))(lambda: clear(high, me.z)),
        clear_far=lambda: pl.when(jnp.logical_not(me.end))(lambda: clear(far, 0)))
    before, plan, after = order_of_work(deep, experts)

    def run(acts):
        for name, *args in acts:
            do[name](*args)

    own_copy.wait()
    run(before)
    for kind, ref in enumerate((wg, wu)):
        pltpu.make_async_copy(ref, ref, weight_sem.at[kind]).wait()
    subs = experts * blocks
    for order in range(deep):
        other_core(order)
        acts = plan[order]
        run(acts.get(-1, []))
        pack(order)

        def body(s, carry, order=order, acts=acts):
            for k in range(subs):
                if acts.get(k):
                    pl.when(s == k)(lambda k=k: run(acts[k]))
            hidden_step(order, s)
            return carry
        lax.fori_loop(0, subs, body, None)
        for t in range(len(tiles)):
            run(acts.get(subs + t, []))
            down_step(order, t)
    run(after)
    assert len(sends) == send_sem.shape[0], len(sends)
    for number, cond, total, cols in sends.values():
        spent = rows_ref.at[pl.ds(0, total), cols]
        when(cond(), lambda: remote(
            spent, spent, send_sem.at[number], own_sem, (me.g, 1 - me.c)).wait_send())


def order_of_work(deep, experts):
    last = deep - 1
    before = [("c_first",), ("z_first", 0), ("z_cross", 0), ("weights",)]
    before += [("clear_low",), ("clear_high",), ("clear_far",)]
    before += [("c_second",), ("turn_down", 0)]
    before += [("z_second", 0), ("z_first", 1), ("z_cross", 1)]
    before += [("turn_down", e) for e in range(1, experts)]
    before += [("c_third",), ("z_third", 0)]
    plan = [{} for _ in range(deep)]

    def put(order, step, *acts):
        plan[min(order, last)].setdefault(step, []).extend(acts)

    put(0, 1, ("z_second", 1))
    for order in range(last):
        if order:
            put(*((1, -1) if order == 1 else (order - 1, 7)), ("z_second", order + 1))
        if order + 2 < deep:
            put(order, 0 if order else 2, ("z_first", order + 2), ("z_cross", order + 2))
        put(order, (2, 5, 4)[order] if deep == 4 else 2, ("c_line", order + 1))
        put(order, (6, 5, 5)[order] if deep == 4 else 5, ("z_third", order + 1))
    if last > 1:
        put(last - 1, 0, ("s_third", 1), ("c_sum", 1, 0))
        for order in range(2, last):
            put(last, 7, ("s_second", order))
        put(last, 7, ("z_sum", 1, 0, 0))
        put(last, -1, ("s_second", 1))
        for order in range(2, last):
            put(last, 0, ("s_third", order), ("c_sum", order, 0))
    else:
        put(last, 0, ("s_third", 0))
    after = [("s_third", last), ("c_sum", last, 0)]
    after += [("c_sum", reach, hop) for reach in range(2, last) for hop in range(1, reach)]
    after += [("c_sum", last, hop) for hop in range(1, 2 if last > 1 else 1)]
    after += [("s_second", last)]
    if last > 1:
        after += [("s_third", 0)]
    after += [("z_sum", reach, 0) for reach in range(2, last)]
    after += [("z_sum", last, 0, 1), ("z_sum", last, 0, 0)]
    if last > 1:
        after += [("z_sum", 1, 0, 1)]
    after += [("c_sum", last, hop) for hop in range(2, last)]
    after += [("z_sum", last, hop, 0) for hop in range(1, 2 if last > 1 else 1)]
    after += [("z_sum", last, hop, 1) for hop in range(1, 2 if last > 1 else 1)]
    after += [("z_sum", reach, hop) for reach in range(2, last) for hop in range(1, reach)]
    after += [("s_second", 0), ("c_back",)]
    after += [("z_sum", last, hop, h) for hop in range(2, last) for h in range(2)]
    after += [("c_cross",), ("z_final",), ("c_final",)]
    return before, plan, after


def fused_body(tokens, gate_weights, expert_ids, w_gate, w_up, w_down):
    columns = lax.axis_size("grp")
    rows, width = tokens.shape
    experts, _, units = w_gate.shape
    deep = columns // 4
    half = rows // 2
    split = max(1, round(width * 2 / 9 / TILE)) * TILE
    split_back = split
    edges = list(range(0, width, 4 * TILE)) + [width]
    tiles = list(zip(edges[:-1], edges[1:]))
    padded = -(-columns * experts // LANES) * LANES
    blocks = units // TILE
    bf16 = tokens.dtype
    depth = 2 * rows * RGROUPS // (columns * experts)
    dma = pltpu.SemaphoreType.DMA
    vmem = lambda *shape: pltpu.VMEM(shape, bf16)
    anywhere = pl.BlockSpec(memory_space=pl.ANY)
    local = pl.BlockSpec(memory_space=pltpu.VMEM)
    lined = columns * rows
    groups = 8 * (deep - 1) + 2 * (deep - 2) + 7
    return pl.pallas_call(
        functools.partial(layer_kernel, columns, split, split_back, depth, tiles),
        out_shape=jax.ShapeDtypeStruct((rows, width), bf16),
        in_specs=[anywhere, local, local, anywhere, anywhere, anywhere],
        out_specs=local,
        scratch_shapes=[
            vmem(2 * lined, width + padded),
            vmem(experts * blocks, width, TILE), vmem(experts * blocks, width, TILE),
            vmem(experts * units, width),
            vmem(8 * rows, experts * 8 * depth), vmem(8 * rows, experts * 8 * depth),
            vmem(experts * 8 * depth, width), vmem(experts * 8 * depth, units),
            vmem(experts * 8 * depth, 4 * TILE),
            vmem(2 * lined, width), vmem(lined, width),
            vmem(deep * 4 * half, width), vmem(deep * rows, width),
            vmem(lined, width), vmem(lined, width),
            vmem(4 * rows, width),
            dma, dma((2,)), dma((experts,)), dma((groups,)), dma((2, columns)), dma((columns,)), dma((2,)),
            dma((deep,)), dma((deep,)), dma((deep, 2, 2)), dma((deep, 2)), dma((deep, 2, 2)), dma((deep, 2, 2)),
            dma((2,)), dma((2, 2)), dma((2,)), dma((columns,)), dma((columns,)),
        ],
        compiler_params=pltpu.CompilerParams(
            collective_id=1, has_side_effects=True, vmem_limit_bytes=54 * 2**20),
        name="expert_layer",
    )(tokens, expert_ids.T, gate_weights.T, w_gate, w_up, w_down)


def expert_rows(inputs, scales, gate_part, up_part, down_part):
    gate_act = jnp.dot(inputs, gate_part, preferred_element_type=jnp.float32)
    upward = jnp.dot(inputs, up_part, preferred_element_type=jnp.float32)
    hidden = (jax.nn.silu(gate_act) * upward).astype(jnp.bfloat16)
    projected = lax.dot_general(
        hidden, down_part, (((1,), (1,)), ((), ())), preferred_element_type=jnp.float32
    )
    return projected * scales.astype(jnp.float32)[:, None]


def weights_path(rows_in, scales_in, w_gate, w_up, w_down):
    row_dims = rows_in.shape
    shard_units = w_gate.shape[2]
    expert_inputs = [rows_in[:, expert].reshape(-1, row_dims[3]) for expert in range(row_dims[1])]
    expert_scales = [scales_in[:, expert].reshape(-1) for expert in range(row_dims[1])]
    starting = tuple(
        (
            jnp.zeros((row_dims[0] * row_dims[2], row_dims[3]), jnp.float32)
            for expert in range(row_dims[1])
        )
    )
    gate_piece = lax.all_gather(w_gate, "loc", axis=2, tiled=True)
    up_piece = lax.all_gather(w_up, "loc", axis=2, tiled=True)
    down_piece = lax.all_gather(w_down, "loc", axis=2, tiled=True)
    updated = []
    for expert in range(row_dims[1]):
        running = starting[expert]
        for block_index in range(gate_piece.shape[2] // shard_units):
            lower_unit = block_index * shard_units
            upper_unit = lower_unit + shard_units
            values = expert_rows(
                expert_inputs[expert],
                expert_scales[expert],
                gate_piece[expert][:, lower_unit:upper_unit],
                up_piece[expert][:, lower_unit:upper_unit],
                down_piece[expert][:, lower_unit:upper_unit],
            )
            rounded = lax.optimization_barrier(values.astype(jnp.bfloat16))
            running = running + rounded.astype(jnp.float32)
        updated.append(running)
    folded = tuple(updated)
    stacked = jnp.stack(
        [folded_part.reshape(row_dims[0], row_dims[2], row_dims[3]) for folded_part in folded],
        axis=1,
    )
    return stacked.astype(jnp.bfloat16)


def slot_body(tokens, gate_weights, expert_ids, w_gate, w_up, w_down):
    tok_count = tokens.shape[0]
    choices_per = expert_ids.shape[1]
    feature_count = tokens.shape[1]
    group_count = lax.axis_size("grp")
    local_experts = w_gate.shape[0]
    expert_total = group_count * local_experts
    slot_depth = 2 * tok_count * RGROUPS // expert_total
    slot_total = expert_total * slot_depth
    pair_ids = expert_ids.reshape(-1)
    pair_count = pair_ids.shape[0]
    pair_order = jnp.arange(pair_count, dtype=jnp.int32)
    same_expert = (pair_ids[:, None] == pair_ids[None, :]).astype(jnp.int32)
    earlier = (pair_order[:, None] > pair_order[None, :]).astype(jnp.int32)
    slot_rank = jnp.sum(same_expert * earlier, axis=1)
    position = pair_ids * slot_depth + slot_rank
    pair_onehot = jnp.arange(slot_total, dtype=jnp.int32)[:, None] == position[None, :]
    placement = jnp.sum(
        pair_onehot.reshape(slot_total, tok_count, choices_per).astype(jnp.int32), axis=2
    ).astype(jnp.bfloat16)
    send_rows = jnp.dot(placement, tokens, preferred_element_type=jnp.float32).astype(jnp.bfloat16)
    flat_scales = gate_weights.reshape(-1).astype(jnp.float32)
    send_scales = jnp.sum(jnp.where(pair_onehot, flat_scales[None, :], 0.0), axis=1).astype(
        jnp.bfloat16
    )
    send_rows = send_rows.reshape(group_count, local_experts, slot_depth, feature_count)
    send_scales = send_scales.reshape(group_count, local_experts, slot_depth)
    computed = weights_path(
        lax.all_to_all(send_rows, "grp", split_axis=0, concat_axis=0, tiled=True),
        lax.all_to_all(send_scales, "grp", split_axis=0, concat_axis=0, tiled=True),
        w_gate,
        w_up,
        w_down,
    )
    returned = lax.all_to_all(computed, "grp", split_axis=0, concat_axis=0, tiled=True)
    flat_back = returned.reshape(slot_total, feature_count)
    mixed_out = lax.dot_general(
        placement, flat_back, (((0,), (0,)), ((), ())), preferred_element_type=jnp.float32
    )
    return mixed_out.astype(jnp.bfloat16)


def body(tokens, gate_weights, expert_ids, w_gate, w_up, w_down):
    tok_count, width = tokens.shape
    units = w_gate.shape[2]
    columns = lax.axis_size("grp")
    slot_depth = 2 * tok_count * RGROUPS // (columns * w_gate.shape[0])
    dense = slot_depth * w_gate.shape[0] >= tok_count
    fits = (columns % 4 == 0 and lax.axis_size("loc") == 2 and tok_count % 32 == 0
            and columns >= 8 and width % TILE == 0 and width > TILE
            and units % TILE == 0 and width % units == 0 and 8 * slot_depth % LANES == 0)
    chosen = fused_body if dense and fits else slot_body
    return chosen(tokens, gate_weights, expert_ids, w_gate, w_up, w_down)


def solution(mesh):
    placed = (
        P(("grp", "loc"), None),
        P(("grp", "loc"), None),
        P(("grp", "loc"), None),
        P("grp", None, "loc"),
        P("grp", None, "loc"),
        P("grp", None, "loc"),
    )
    return jax.shard_map(
        body, mesh=mesh, in_specs=placed, out_specs=P(("grp", "loc"), None), check_vma=False
    )
```
